32 devices in a mesh: dp: 4 (over z), ep: 8 (over y, x, core).
Axes of the slice: x: 2, y: 2, z: 4, core: 2. Of those that a mesh axis runs over, the one named last changes fastest.
Arguments:
- x_in: bfloat16 [32, 256, 1536], P(('dp', 'ep'))
- dy_in: bfloat16 [32, 256, 1536], P(('dp', 'ep'))
- route_idx: int32 [32, 256, 6], P(('dp', 'ep'))
- gain_attn: bfloat16 [1536], replicated
- w_qkv: bfloat16 [1536, 4608], replicated
- w_o: bfloat16 [1536, 1536], replicated
- gain_ffn: bfloat16 [1536], replicated
- w_router: bfloat16 [1536, 64], replicated
- w_up: bfloat16 [64, 1536, 512], P('ep')
- w_lin: bfloat16 [64, 1536, 512], P('ep')
- w_down: bfloat16 [64, 512, 1536], P('ep')
Outputs:
- output 1: bfloat16 [32, 256, 1536], P(('dp', 'ep'))
- output 2: float32 [1536], replicated
- output 3: float32 [1536, 4608], replicated
- output 4: float32 [1536, 1536], replicated
- output 5: float32 [1536], replicated
- output 6: float32 [1536, 64], replicated
- output 7: float32 [64, 1536, 512], P('ep')
- output 8: float32 [64, 1536, 512], P('ep')
- output 9: float32 [64, 512, 1536], P('ep')
All inputs are finite; a program needn't handle non-finite values.
Results may differ from the reference program's by a relative error of at most 0.017496.
Values are sent between devices in bfloat16 or wider.
A program may use at most 1 GiB of HBM per device.

```python
import jax
import jax.numpy as jnp
from jax import lax

D = 1536
FF = 512
EXPERTS = 64
TOP = 6
SEQ = 256
SEQS_DEV = 1
DEVICES = 32
CAP = 32
HEAD = 128

HEADS = D // HEAD
TOKENS = SEQS_DEV * SEQ
EPS = 1e-6


def setup_inputs(seed: int = 0) -> dict:
    keys = jax.random.split(jax.random.key(seed), 12)
    batch = SEQS_DEV * DEVICES
    all_tokens = batch * SEQ
    score_rows = jax.random.randint(keys[2], (all_tokens, EXPERTS), 0, 1024)
    expert_bias = jax.random.randint(keys[3], (EXPERTS,), 0, 160)
    ranked = (score_rows + expert_bias[None, :]) * EXPERTS + jnp.arange(EXPERTS)[None, :]
    route_idx = lax.top_k(ranked, TOP)[1].astype(jnp.int32).reshape(batch, SEQ, TOP)
    x_in = jax.random.normal(keys[0], (batch, SEQ, D), jnp.float32)
    dy_in = jax.random.normal(keys[1], (batch, SEQ, D), jnp.float32)
    gain_attn = 1.0 + 0.3 * jax.random.normal(keys[4], (D,), jnp.float32)
    w_qkv = jax.random.normal(keys[5], (D, 3 * D), jnp.float32) * D ** -0.5
    w_o = jax.random.normal(keys[6], (D, D), jnp.float32) * D ** -0.5
    gain_ffn = 1.0 + 0.3 * jax.random.normal(keys[7], (D,), jnp.float32)
    w_router = jax.random.normal(keys[8], (D, EXPERTS), jnp.float32) * 2.0 * D ** -0.5
    w_up = jax.random.normal(keys[9], (EXPERTS, D, FF), jnp.float32) * D ** -0.5
    w_lin = jax.random.normal(keys[10], (EXPERTS, D, FF), jnp.float32) * D ** -0.5
    w_down = jax.random.normal(keys[11], (EXPERTS, FF, D), jnp.float32) * FF ** -0.5
    return {
        'x_in': x_in.astype(jnp.bfloat16),
        'dy_in': dy_in.astype(jnp.bfloat16),
        'route_idx': route_idx,
        'gain_attn': gain_attn.astype(jnp.bfloat16),
        'w_qkv': w_qkv.astype(jnp.bfloat16),
        'w_o': w_o.astype(jnp.bfloat16),
        'gain_ffn': gain_ffn.astype(jnp.bfloat16),
        'w_router': w_router.astype(jnp.bfloat16),
        'w_up': w_up.astype(jnp.bfloat16),
        'w_lin': w_lin.astype(jnp.bfloat16),
        'w_down': w_down.astype(jnp.bfloat16),
    }


def rms_norm(values, gain):
    scale = lax.rsqrt(jnp.mean(values * values, axis=-1, keepdims=True) + EPS)
    return (values * scale * gain).astype(jnp.bfloat16)


def attn_core(qkv_rows):
    seq_len = qkv_rows.shape[0]
    split = qkv_rows.astype(jnp.float32).reshape(seq_len, 3, HEADS, HEAD)
    scores = jnp.einsum('qhc,khc->hqk', split[:, 0], split[:, 1]) * (HEAD ** -0.5)
    causal = jnp.arange(seq_len)[:, None] >= jnp.arange(seq_len)[None, :]
    scores = jnp.where(causal[None], scores, -1e30)
    prob_rows = jax.nn.softmax(scores, axis=-1).astype(jnp.bfloat16).astype(jnp.float32)
    mixed = jnp.einsum('hqk,khc->qhc', prob_rows, split[:, 2])
    return mixed.astype(jnp.bfloat16).reshape(seq_len, D)


def gate_weights(logits, idx_rows):
    prob_rows = jax.nn.softmax(logits, axis=-1)
    picked = jnp.take_along_axis(prob_rows, idx_rows, axis=-1)
    return picked / jnp.sum(picked, axis=-1, keepdims=True)


def route_tables(idx_rows):
    onehot = (idx_rows[:, :, None] == jnp.arange(EXPERTS)[None, None, :]).astype(jnp.int32)
    counts = jnp.sum(onehot, axis=1)
    prior = jnp.cumsum(counts, axis=0) - counts
    position = jnp.sum(onehot * prior[:, None, :], axis=-1)
    slot = jnp.where(position < CAP, idx_rows * CAP + position, EXPERTS * CAP)
    flat_ids = jnp.arange(TOKENS * TOP, dtype=jnp.int32)
    src_id = jnp.full((EXPERTS * CAP + 1,), TOKENS * TOP, jnp.int32).at[slot.reshape(-1)].set(flat_ids)
    return slot, src_id[:EXPERTS * CAP] // TOP


def dev_forward(x_dev, idx_rows, params):
    gain_one, wqkv_f, wout_f, gain_two, router_f, up_f, lin_f, down_f = params
    xn_one = rms_norm(x_dev, gain_one)
    qkv_all = jnp.einsum('bsd,de->bse', xn_one.astype(jnp.float32), wqkv_f).astype(jnp.bfloat16)
    attn_out = jax.vmap(attn_core)(qkv_all)
    attn_proj = jnp.einsum('bsd,de->bse', attn_out.astype(jnp.float32), wout_f)
    hidden = (x_dev + attn_proj).astype(jnp.bfloat16).astype(jnp.float32).reshape(TOKENS, D)
    xn_two = rms_norm(hidden, gain_two).astype(jnp.float32)
    gates = gate_weights(jnp.dot(xn_two, router_f), idx_rows)
    slot, src_tok = route_tables(idx_rows)
    x_pad = jnp.concatenate([xn_two, jnp.zeros((1, D), jnp.float32)], axis=0)
    buffer = x_pad[src_tok].astype(jnp.bfloat16).astype(jnp.float32).reshape(EXPERTS, CAP, D)
    up_gate = jnp.einsum('ecd,edf->ecf', buffer, up_f).astype(jnp.bfloat16).astype(jnp.float32)
    up_lin = jnp.einsum('ecd,edf->ecf', buffer, lin_f).astype(jnp.bfloat16).astype(jnp.float32)
    act_rows = (jax.nn.silu(up_gate) * up_lin).astype(jnp.bfloat16).astype(jnp.float32)
    y_exp = jnp.einsum('ecf,efd->ecd', act_rows, down_f).astype(jnp.bfloat16).astype(jnp.float32)
    y_pad = jnp.concatenate([y_exp.reshape(EXPERTS * CAP, D), jnp.zeros((1, D), jnp.float32)], axis=0)
    y_sel = y_pad[slot]
    moe_out = jnp.sum(gates[:, :, None] * y_sel, axis=1)
    return (hidden + moe_out).astype(jnp.bfloat16).reshape(SEQS_DEV, SEQ, D)


def reference(x_in, dy_in, route_idx, gain_attn, w_qkv, w_o, gain_ffn, w_router, w_up, w_lin, w_down):
    params = tuple(arr.astype(jnp.float32) for arr in (gain_attn, w_qkv, w_o, gain_ffn, w_router, w_up, w_lin, w_down))
    x_all = x_in.astype(jnp.float32).reshape(DEVICES, SEQS_DEV, SEQ, D)
    idx_all = route_idx.reshape(DEVICES, TOKENS, TOP)
    dev_step = jax.checkpoint(dev_forward)

    def layer(x_stack, prm):
        return lax.map(lambda pair: dev_step(pair[0], pair[1], prm), (x_stack, idx_all))

    out_val, pull = jax.vjp(layer, x_all, params)
    dx_all, grads = pull(dy_in.reshape(DEVICES, SEQS_DEV, SEQ, D))
    grad_g1, grad_wqkv, grad_wo, grad_g2, grad_wr, grad_up, grad_lin, grad_down = grads
    return (dx_all.astype(jnp.bfloat16).reshape(x_in.shape), grad_g1, grad_wqkv, grad_wo, grad_g2, grad_wr, grad_up, grad_lin, grad_down)
```

```python
import jax
import jax.numpy as jnp
from jax import lax
from jax.sharding import PartitionSpec as P


EPS = 1e-6
HEAD = 128
DROPPED = 64.0
UNCHOSEN = 128.0
F32 = jnp.float32
BF16 = jnp.bfloat16


def mm(spec, a, b):
    return jnp.einsum(spec, a, b, preferred_element_type=F32)


def rms_norm(values, gain):
    scale = lax.rsqrt(jnp.mean(values * values, axis=-1, keepdims=True) + EPS)
    return (values * scale * gain).astype(BF16)


def attn_core(qkv_rows):
    num_seqs, seq_len, width = qkv_rows.shape
    heads = width // (3 * HEAD)
    split = qkv_rows.reshape(num_seqs, seq_len, 3, heads, HEAD)
    scores = mm('bqhc,bkhc->bhqk', split[:, :, 0], split[:, :, 1]) * (HEAD ** -0.5)
    rows = lax.broadcasted_iota(jnp.int32, (seq_len, seq_len), 0)
    cols = lax.broadcasted_iota(jnp.int32, (seq_len, seq_len), 1)
    scores = jnp.where(rows >= cols, scores, -1e30)
    prob_rows = jax.nn.softmax(scores, axis=-1).astype(BF16)
    mixed = mm('bhqk,bkhc->bqhc', prob_rows, split[:, :, 2])
    return mixed.astype(BF16).reshape(num_seqs, seq_len, heads * HEAD)


def swiglu(gate_in, lin_in):
    return (jax.nn.silu(gate_in.astype(F32)) * lin_in.astype(F32)).astype(BF16)


def slot_codes(idx_rows, experts, cap):
    tokens = idx_rows.shape[0]
    chosen = jnp.any(idx_rows[:, :, None] == jnp.arange(experts, dtype=jnp.int32), axis=1).astype(BF16)
    rows = lax.broadcasted_iota(jnp.int32, (tokens, tokens), 0)
    cols = lax.broadcasted_iota(jnp.int32, (tokens, tokens), 1)
    prior = mm('se,st->et', chosen, (rows < cols).astype(BF16))
    taken = mm('se,st->et', chosen, (rows == cols).astype(BF16))
    return jnp.where(taken > 0.5, jnp.where(prior < cap, prior, DROPPED), UNCHOSEN).astype(BF16)


def one_hot(codes, cap):
    slots = lax.broadcasted_iota(jnp.int32, codes.shape[:-1] + (cap, codes.shape[-1]), codes.ndim - 1)
    return (codes[..., None, :].astype(F32) == slots.astype(F32)).astype(BF16)


def gates_of(xn, codes, w_router):
    logits = mm('...td,de->...et', xn, w_router)
    prob = jax.nn.softmax(logits, axis=-2)
    mask = (codes.astype(F32) < UNCHOSEN - 1.0).astype(F32)
    picked = prob * mask
    total = jnp.sum(picked, axis=-2, keepdims=True)
    return prob, mask, picked / total, total


def dispatch(select, rows):
    return mm('sect,std->secd', select, rows).astype(BF16)


def expert_core(select, gate_rows, xn, dy, w_up, w_lin, w_down):
    recv = dispatch(select, xn)
    dy_rows = dispatch(select, dy)
    gate_slot = jnp.sum(select.astype(F32) * gate_rows[:, :, None, :], axis=-1, keepdims=True)
    d_recv = (gate_slot * dy_rows.astype(F32)).astype(BF16)
    up_gate = mm('secd,edf->secf', recv, w_up).astype(BF16)
    up_lin = mm('secd,edf->secf', recv, w_lin).astype(BF16)
    act_rows, act_pull = jax.vjp(swiglu, up_gate, up_lin)
    d_act = mm('secd,efd->secf', d_recv, w_down).astype(BF16)
    d_gate_in, d_lin_in = act_pull(d_act)
    return recv, dy_rows, d_recv, act_rows, d_gate_in, d_lin_in


def sum_everywhere(value, world):
    piece = lax.psum_scatter(value, world, scatter_dimension=0, tiled=True)
    return lax.all_gather(piece, world, axis=0, tiled=True)


def after(value, *deps):
    return lax.optimization_barrier((value,) + deps)[0]


def solution(mesh):
    tok_spec = P(('dp', 'ep'))
    exp_spec = P('ep')
    rep_spec = P()
    world = ('dp', 'ep')

    def local(x_in, dy_in, route_idx, gain_attn, w_qkv, w_o, gain_ffn, w_router, w_up, w_lin, w_down):
        num_seqs, seq_len, width = x_in.shape
        tokens = num_seqs * seq_len
        top = route_idx.shape[-1]
        experts = w_router.shape[1]
        local_exp = w_up.shape[0]
        cap = ((tokens * top * 5) // (experts * 4) + 7) // 8 * 8
        my_dp, my_ep = lax.axis_index('dp'), lax.axis_index('ep')
        ep_size = mesh.shape['ep']

        codes = slot_codes(route_idx.reshape(tokens, top), experts, cap)
        dy_own = dy_in.reshape(tokens, width)
        codes_all = lax.all_gather(codes, world)
        dy_plane = lax.all_gather(dy_own, 'ep')

        x_f = x_in.astype(F32)
        xn_one, norm_one_pull = jax.vjp(rms_norm, x_f, gain_attn.astype(F32))
        qkv_all = mm('bsd,de->bse', xn_one, w_qkv).astype(BF16)
        attn_out, attn_pull = jax.vjp(attn_core, qkv_all)
        attn_proj = mm('bsd,de->bse', attn_out, w_o)
        hidden = (x_f + attn_proj).astype(BF16).astype(F32).reshape(tokens, width)
        xn_two, norm_two_pull = jax.vjp(rms_norm, hidden, gain_ffn.astype(F32))

        xn_plane = lax.all_gather(after(xn_two, dy_plane, codes_all), 'ep')
        dy_all = lax.all_gather(after(dy_own, xn_plane), world)
        xn_all = lax.all_gather(after(xn_two, xn_plane), world)

        mine = lambda arr: lax.dynamic_slice_in_dim(arr, my_ep * local_exp, local_exp, axis=1)
        codes_plane = lax.dynamic_slice_in_dim(codes_all, my_dp * ep_size, ep_size, axis=0)
        _, _, gates_plane, _ = gates_of(xn_plane, codes_plane, w_router)
        recv, dy_rows, d_recv, act_rows, d_gate_in, d_lin_in = expert_core(
            one_hot(mine(codes_plane), cap), mine(gates_plane), xn_plane, dy_plane, w_up, w_lin, w_down)
        y_exp = mm('secf,efd->secd', act_rows, w_down).astype(BF16)
        d_gate_rows = jnp.sum(dy_rows.astype(F32) * y_exp.astype(F32), axis=-1)
        d_gate_back = lax.all_to_all(d_gate_rows, 'ep', 0, 0).reshape(experts, cap)
        d_tok_exp = (mm('secf,edf->secd', d_gate_in, w_up) + mm('secf,edf->secd', d_lin_in, w_lin)).astype(BF16)
        d_back = lax.all_to_all(d_tok_exp, 'ep', 0, 0).reshape(experts, cap, width)

        select_own = one_hot(codes, cap)
        d_moe_in = mm('ect,ecd->td', select_own, d_back)
        prob, mask, gates, total = gates_of(xn_two, codes, w_router)
        d_gates = jnp.sum(select_own.astype(F32) * d_gate_back[:, :, None], axis=1)
        d_picked = (d_gates - jnp.sum(d_gates * gates, axis=0, keepdims=True)) / total * mask
        d_logits = (prob * (d_picked - jnp.sum(prob * d_picked, axis=0, keepdims=True))).astype(BF16)
        d_xn_two = (d_moe_in + mm('et,de->td', d_logits, w_router)).astype(BF16)
        grad_router = mm('td,et->de', xn_two, d_logits)
        grad_router = lax.psum(grad_router, world)
        d_hidden, grad_gain_ffn = norm_two_pull(d_xn_two)
        d_resid = (d_hidden + dy_own.astype(F32)).astype(BF16).reshape(num_seqs, seq_len, width)
        grad_wo = mm('bsd,bse->de', attn_out, d_resid)
        d_attn_out = mm('bse,de->bsd', d_resid, w_o).astype(BF16)
        grad_wo = sum_everywhere(grad_wo, world)
        d_qkv = attn_pull(d_attn_out)[0]
        grad_wqkv = mm('bsd,bse->de', xn_one, d_qkv)
        piece_wqkv = lax.psum_scatter(grad_wqkv, world, scatter_dimension=0, tiled=True)
        grad_wqkv = lax.all_gather(piece_wqkv, world, axis=0, tiled=True)
        d_xn_one = mm('bse,de->bsd', d_qkv, w_qkv).astype(BF16)
        d_x_norm, grad_gain_attn = norm_one_pull(d_xn_one)
        dx_out = (d_x_norm + d_resid.astype(F32)).astype(BF16)
        grad_gain_attn, grad_gain_ffn = lax.psum((grad_gain_attn, grad_gain_ffn), world)

        xn_late = after(xn_all, d_qkv)
        _, _, gates_all, _ = gates_of(xn_late, codes_all, w_router)
        recv, dy_rows, d_recv, act_rows, d_gate_in, d_lin_in = expert_core(
            one_hot(mine(codes_all), cap), mine(gates_all), xn_late, dy_all, w_up, w_lin, w_down)
        grad_down = mm('secf,secd->efd', act_rows, d_recv)
        grad_up = mm('secd,secf->edf', recv, d_gate_in)
        grad_lin = mm('secd,secf->edf', recv, d_lin_in)
        return (dx_out, grad_gain_attn, grad_wqkv, grad_wo, grad_gain_ffn, grad_router, grad_up, grad_lin, grad_down)

    in_specs = (tok_spec, tok_spec, tok_spec, rep_spec, rep_spec, rep_spec, rep_spec, rep_spec, exp_spec, exp_spec, exp_spec)
    out_specs = (tok_spec, rep_spec, rep_spec, rep_spec, rep_spec, rep_spec, exp_spec, exp_spec, exp_spec)

    return jax.shard_map(local, mesh=mesh, in_specs=in_specs, out_specs=out_specs, check_vma=False)
```

```python
import functools

import jax
import jax.numpy as jnp
from jax import lax
from jax.experimental import pallas as pl
from jax.experimental.pallas import tpu as pltpu
from jax.sharding import PartitionSpec as P


EPS = 1e-6
HEAD = 128
DROPPED = 64.0
UNCHOSEN = 128.0
F32 = jnp.float32
BF16 = jnp.bfloat16


def mm(spec, a, b):
    return jnp.einsum(spec, a, b, preferred_element_type=F32)


def rms_norm(values, gain):
    scale = lax.rsqrt(jnp.mean(values * values, axis=-1, keepdims=True) + EPS)
    return (values * scale * gain).astype(BF16)


def attn_core(qkv_rows):
    num_seqs, seq_len, width = qkv_rows.shape
    heads = width // (3 * HEAD)
    split = qkv_rows.reshape(num_seqs, seq_len, 3, heads, HEAD)
    scores = mm('bqhc,bkhc->bhqk', split[:, :, 0], split[:, :, 1]) * (HEAD ** -0.5)
    rows = lax.broadcasted_iota(jnp.int32, (seq_len, seq_len), 0)
    cols = lax.broadcasted_iota(jnp.int32, (seq_len, seq_len), 1)
    scores = jnp.where(rows >= cols, scores, -1e30)
    prob_rows = jax.nn.softmax(scores, axis=-1).astype(BF16)
    mixed = mm('bhqk,bkhc->bqhc', prob_rows, split[:, :, 2])
    return mixed.astype(BF16).reshape(num_seqs, seq_len, heads * HEAD)


def slot_codes(idx_rows, experts, cap):
    tokens = idx_rows.shape[0]
    chosen = jnp.any(idx_rows[:, :, None] == jnp.arange(experts, dtype=jnp.int32), axis=1).astype(BF16)
    rows = lax.broadcasted_iota(jnp.int32, (tokens, tokens), 0)
    cols = lax.broadcasted_iota(jnp.int32, (tokens, tokens), 1)
    prior = mm('se,st->et', chosen, (rows < cols).astype(BF16))
    taken = mm('se,st->et', chosen, (rows == cols).astype(BF16))
    return jnp.where(taken > 0.5, jnp.where(prior < cap, prior, DROPPED), UNCHOSEN).astype(BF16)


def one_hot(codes, cap):
    slots = lax.broadcasted_iota(jnp.int32, codes.shape[:-1] + (cap, codes.shape[-1]), codes.ndim - 1)
    return (codes[..., None, :].astype(F32) == slots.astype(F32)).astype(BF16)


def gates_of(xn, codes, w_router):
    logits = mm('...td,de->...et', xn, w_router)
    prob = jax.nn.softmax(logits, axis=-2)
    mask = (codes.astype(F32) < UNCHOSEN - 1.0).astype(F32)
    picked = prob * mask
    total = jnp.sum(picked, axis=-2, keepdims=True)
    return prob, mask, picked / total, total


def after(value, *deps):
    return lax.optimization_barrier((value,) + deps)[0]


HALF = 768
CHUNK = 128
STEPS = HALF // CHUNK
MESH = pl.DeviceIdType.MESH


def dot_tn(a, b):
    return lax.dot_general(a, b, (((0,), (0,)), ((), ())), preferred_element_type=jnp.float32)


def dense_kernel(xn_ref, ao_ref, dsend_ref, gains_ref, low_ref, high_ref, gains_out_ref,
                 dall, part, z_in, total, gain_buf,
                 d_send, d_recv, dp_send, dp_recv, z_send, z_recv, own_sem, g_send, g_recv):
    z = lax.axis_index('dp')
    ep = lax.axis_index('ep')
    core = lax.rem(ep, 2)
    quarter = ep // 2
    width = dsend_ref.shape[2]
    split = width * 3 // 4
    tokens = dsend_ref.shape[1]
    partner = ep + 1 - 2 * core
    bit_x = lax.rem(quarter, 2)
    bit_y = quarter // 2
    flip = lambda bx, by: 2 * ((bit_x + bx - 2 * bit_x * bx) + 2 * (bit_y + by - 2 * bit_y * by)) + core
    x_dev, y_dev, xy_dev = flip(1, 0), flip(0, 1), flip(1, 1)
    inner = jnp.logical_or(z == 1, z == 2)
    z_mate = jnp.where(z == 0, 1, jnp.where(z == 1, 0, jnp.where(z == 2, 3, 2)))
    z_cross = 3 - z

    def copy(src, dst, s_sem, r_sem, dp, e):
        return pltpu.make_async_remote_copy(src_ref=src, dst_ref=dst, send_sem=s_sem, recv_sem=r_sem,
                                            device_id=(dp, e), device_id_type=MESH)

    rows_of = lambda e: pl.ds(pl.multiple_of(e * tokens, tokens), tokens)
    far = (x_dev, y_dev, xy_dev)
    for i, dev in enumerate(far):
        copy(dsend_ref.at[dev // 2], dall.at[rows_of(ep)], d_send.at[i], d_recv.at[i], z, dev).start()
    copy(dsend_ref.at[quarter], dall.at[rows_of(ep)], dp_send.at[3], dp_recv.at[3], z, partner).start()

    world = 32
    me = z * 8 + ep

    def gain_copy(d, target):
        return copy(gains_ref, gain_buf.at[d], g_send.at[d], g_recv.at[d], target // 8, lax.rem(target, 8))

    def gain_start(d, _):
        gain_copy(d, lax.rem(me + d, world)).start()
        return 0

    lax.fori_loop(1, world, gain_start, 0)

    dall[rows_of(ep), :] = dsend_ref[quarter]
    for i, dev in enumerate(far):
        copy(dsend_ref.at[dev // 2], dall.at[rows_of(dev)], d_send.at[i], d_recv.at[i], z, dev).wait_recv()
        copy(dall.at[rows_of(dev)], dall.at[rows_of(dev)], dp_send.at[i], dp_recv.at[i], z, partner).start()
    for i, dev in enumerate(far + (ep,)):
        other = dev + 1 - 2 * core
        copy(dsend_ref.at[0], dall.at[rows_of(other)], dp_send.at[i], dp_recv.at[i], z, partner).wait_recv()

    up_copy = lambda k: copy(part.at[k], z_in.at[k], z_send.at[0, k], z_recv.at[0, k], z_mate, ep)
    cross_copy = lambda k: copy(part.at[k], total.at[k], z_send.at[1, k], z_recv.at[1, k], z_cross, ep)
    down_copy = lambda k: copy(total.at[k], total.at[k], z_send.at[2, k], z_recv.at[2, k], z_mate, ep)

    def own_copy(k):
        ref = low_ref if k < STEPS // 2 else high_ref
        return pltpu.make_async_copy(total.at[k], ref.at[pl.ds(k % (STEPS // 2) * CHUNK, CHUNK), :], own_sem.at[k])

    for i in range(STEPS + 3):
        k = i
        if k < STEPS:
            cols = slice(k * CHUNK, (k + 1) * CHUNK)
            part[k, :, :split] = dot_tn(xn_ref[:, cols], dall[:, :split])
            part[k, :, split:] = dot_tn(ao_ref[:, cols], dall[:, split:])
        a = i - 1
        t = i - 2

        @pl.when(inner)
        def _():
            if 0 <= a < STEPS:
                up_copy(a).wait_recv()
                part[a] = part[a] + z_in[a]
            if 0 <= t < STEPS:
                cross_copy(t).wait_recv()
                total[t] = part[t] + total[t]
            if 0 <= a < STEPS:
                cross_copy(a).start()
            if 0 <= t < STEPS:
                down_copy(t).start()
                own_copy(t).start()

        @pl.when(jnp.logical_not(inner))
        def _():
            if k < STEPS:
                up_copy(k).start()
            if 0 <= i - 3 < STEPS:
                down_copy(i - 3).wait_recv()
                own_copy(i - 3).start()

    for k in range(STEPS):
        own_copy(k).wait()

    @pl.when(inner)
    def _():
        for k in range(STEPS):
            cross_copy(k).wait_send()
            down_copy(k).wait_send()

    @pl.when(jnp.logical_not(inner))
    def _():
        for k in range(STEPS):
            up_copy(k).wait_send()

    for i, dev in enumerate(far):
        copy(dsend_ref.at[dev // 2], dall.at[rows_of(ep)], d_send.at[i], d_recv.at[i], z, dev).wait_send()
        copy(dall.at[rows_of(dev)], dall.at[rows_of(dev)], dp_send.at[i], dp_recv.at[i], z, partner).wait_send()
    copy(dsend_ref.at[quarter], dall.at[rows_of(ep)], dp_send.at[3], dp_recv.at[3], z, partner).wait_send()

    def gain_wait(d, _):
        gain_copy(d, me).wait()
        return 0

    lax.fori_loop(1, world, gain_wait, 0)
    gain_buf[0] = gains_ref[...]

    def gain_add(s, acc):
        d = lax.rem(me - s + world, world)
        return acc + gain_buf[d]

    gains_out_ref[...] = lax.fori_loop(0, world, gain_add, jnp.zeros(gains_ref.shape, jnp.float32))


def dense_sums(xn, ao, dsend, gains):
    rows, width = xn.shape[0], dsend.shape[2]
    any_spec = pl.BlockSpec(memory_space=pl.ANY)
    vmem = pl.BlockSpec(memory_space=pltpu.VMEM)
    dma = pltpu.SemaphoreType.DMA
    half = jax.ShapeDtypeStruct((HALF // 2, width), jnp.float32)
    return pl.pallas_call(
        dense_kernel,
        out_shape=(half, half, jax.ShapeDtypeStruct(gains.shape, jnp.float32)),
        in_specs=[vmem, vmem, vmem, vmem],
        out_specs=(any_spec, any_spec, vmem),
        scratch_shapes=[
            pltpu.VMEM((rows, width), jnp.bfloat16),
            pltpu.VMEM((STEPS, CHUNK, width), jnp.float32),
            pltpu.VMEM((STEPS, CHUNK, width), jnp.float32),
            pltpu.VMEM((STEPS, CHUNK, width), jnp.float32),
            pltpu.VMEM((32,) + gains.shape, jnp.float32),
            dma((3,)), dma((3,)), dma((4,)), dma((4,)), dma((3, STEPS)), dma((3, STEPS)), dma((STEPS,)), dma((32,)), dma((32,)),
        ],
        compiler_params=pltpu.CompilerParams(has_side_effects=True, vmem_limit_bytes=48 << 20),
        cost_estimate=pl.CostEstimate(flops=100 * 10**9, bytes_accessed=40 << 20, transcendentals=0),
        name='dense_sums',
    )(xn, ao, dsend, gains)


def assemble_kernel(*refs):
    pieces, (qkv_ref, wo_ref, buf, in_sem, out_sem) = refs[:16], refs[16:]
    ep = lax.axis_index('ep')
    bits = (lax.rem(ep, 2), lax.rem(ep // 2, 2), ep // 4)
    size = HALF // 2
    width = buf.shape[2]
    split = width * 3 // 4

    def load(n):
        return pltpu.make_async_copy(pieces[n], buf.at[n % 4], in_sem.at[n % 4])

    def stores(n):
        flips = (n // 2 % 2, n // 4 % 2, n // 8)
        core, bx, by = [b + f - 2 * b * f for b, f in zip(bits, flips)]
        rows = pl.ds(pl.multiple_of(core * HALF + n % 2 * size, size), size)
        q = bx + 2 * by
        return [pltpu.make_async_copy(buf.at[n % 4, :, pl.ds(lo, cols)],
                                      ref.at[rows, pl.ds(pl.multiple_of(q * cols, 128), cols)], out_sem.at[n % 4, i])
                for i, (ref, lo, cols) in enumerate(((qkv_ref, 0, split), (wo_ref, split, width - split)))]

    for n in range(16 + 2):
        if n < 16:
            if n >= 4:
                for c in stores(n - 4):
                    c.wait()
            load(n).start()
        if n >= 2:
            load(n - 2).wait()
            for c in stores(n - 2):
                c.start()
    for n in range(12, 16):
        for c in stores(n):
            c.wait()


def assemble(pieces):
    width = pieces[0].shape[1]
    any_spec = pl.BlockSpec(memory_space=pl.ANY)
    return pl.pallas_call(
        assemble_kernel,
        out_shape=(jax.ShapeDtypeStruct((2 * HALF, 3 * width), F32), jax.ShapeDtypeStruct((2 * HALF, width), F32)),
        in_specs=[any_spec] * 16,
        out_specs=(any_spec, any_spec),
        scratch_shapes=[pltpu.VMEM((4, HALF // 2, width), F32), pltpu.SemaphoreType.DMA((4,)), pltpu.SemaphoreType.DMA((4, 2))],
        compiler_params=pltpu.CompilerParams(vmem_limit_bytes=24 << 20),
        cost_estimate=pl.CostEstimate(flops=20 * 10**9, bytes_accessed=80 << 20, transcendentals=0),
        name='assemble',
    )(*pieces)


def dot_nn(a, b):
    return lax.dot_general(a, b, (((1,), (0,)), ((), ())), preferred_element_type=jnp.float32)


def dot_nt(a, b):
    return lax.dot_general(a, b, (((1,), (1,)), ((), ())), preferred_element_type=jnp.float32)


def slot_select(codes_t, gates, first, local_exp, cap, codes_buf, gates_buf):
    tokens = codes_t.shape[1]
    codes_buf[...] = codes_t
    gates_buf[...] = gates
    my_codes = codes_buf[pl.ds(first, local_exp), :]
    my_gates = gates_buf[pl.ds(first, local_exp), :]
    slots = lax.broadcasted_iota(jnp.int32, (local_exp, cap, tokens), 1).astype(F32)
    select = jnp.where(my_codes[:, None, :] == slots, 1.0, 0.0)
    gate_slot = jnp.sum(select * my_gates[:, None, :], axis=-1, keepdims=True).reshape(local_exp * cap, 1)
    return select.reshape(local_exp * cap, tokens).astype(BF16), gate_slot


def slot_rows(xn, dyc, router, first, local_exp, cap, codes_buf, gates_buf):
    experts = router.shape[0]
    width = xn.shape[1]
    codes = dyc[:, width:].astype(F32).T[:experts]
    logits = dot_nt(router, xn)
    prob = jnp.exp(logits - jnp.max(logits, axis=0, keepdims=True))
    prob = prob / jnp.sum(prob, axis=0, keepdims=True)
    picked = jnp.where(codes < UNCHOSEN - 1.0, prob, 0.0)
    gates = picked / jnp.sum(picked, axis=0, keepdims=True)
    select, gate_slot = slot_select(codes, gates, first, local_exp, cap, codes_buf, gates_buf)
    return dot_nn(select, xn).astype(BF16), dot_nn(select, dyc[:, :width]), gate_slot


def dispatch_kernel(local_exp, cap, place_ref, xn_ref, dyc_ref, router_ref, recv_in, d_recv_in, recv_ref, d_recv_ref, codes_buf, gates_buf):
    first = pl.multiple_of(lax.axis_index('ep') * local_exp, local_exp)
    router = router_ref[...]
    width = xn_ref.shape[2]
    for i in range(xn_ref.shape[0]):
        recv, dy_rows, gate_slot = slot_rows(xn_ref[i], dyc_ref[i], router, first, local_exp, cap, codes_buf.at[i], gates_buf.at[i])
        at = slice(i * cap, (i + 1) * cap)
        recv_ref[:, at, :] = recv.reshape(local_exp, cap, width)
        d_recv_ref[:, at, :] = (gate_slot * dy_rows).astype(BF16).reshape(local_exp, cap, width)


def dispatch_rows(place, xn, dyc, router_t, recv, d_recv, cap):
    planes, sources, tokens, lanes = dyc.shape
    local_exp, _, width = recv.shape
    experts = router_t.shape[0]
    step = 4
    any_spec = pl.BlockSpec(memory_space=pl.ANY)
    plane = lambda r, t: lax.rem(t[0] + r + 1, planes)
    out_spec = pl.BlockSpec((local_exp, step * cap, width), lambda r, s, t: (0, (r + 1) * (sources // step) + s, 0))
    same = lambda arr: jax.ShapeDtypeStruct(arr.shape, arr.dtype)
    return pl.pallas_call(
        functools.partial(dispatch_kernel, local_exp, cap),
        grid_spec=pltpu.PrefetchScalarGridSpec(
            num_scalar_prefetch=1,
            grid=(planes - 1, sources // step),
            in_specs=[pl.BlockSpec((None, step, tokens, width), lambda r, s, t: (plane(r, t), s, 0, 0)),
                      pl.BlockSpec((None, step, tokens, lanes), lambda r, s, t: (plane(r, t), s, 0, 0)),
                      pl.BlockSpec(router_t.shape, lambda r, s, t: (0, 0)), any_spec, any_spec],
            out_specs=(out_spec, out_spec),
            scratch_shapes=[pltpu.VMEM((step, experts, tokens), F32), pltpu.VMEM((step, experts, tokens), F32)]),
        out_shape=(same(recv), same(d_recv)),
        input_output_aliases={4: 0, 5: 1},
        compiler_params=pltpu.CompilerParams(vmem_limit_bytes=56 << 20),
        cost_estimate=pl.CostEstimate(flops=planes * sources * 4 * local_exp * cap * tokens * width, transcendentals=0,
                                      bytes_accessed=planes * sources * tokens * width * 8),
        name='dispatch_rows',
    )(place, xn, dyc, router_t, recv, d_recv)


def hidden_grads(recv, d_recv, up, lin, down):
    u = dot_nn(recv, up).astype(BF16).astype(F32)
    v = dot_nn(recv, lin).astype(BF16).astype(F32)
    d_act = dot_nt(d_recv, down).astype(BF16).astype(F32)
    sig = jax.nn.sigmoid(u)
    act = u * sig
    d_u = d_act * v * (sig + act * (1.0 - sig))
    return (act * v).astype(BF16), d_u.astype(BF16), (d_act * act).astype(BF16)


def moe_kernel(cap, xn_ref, dyc_ref, router_ref, up_ref, lin_ref, down_ref, back_ref, gate_back_ref, recv_out, d_recv_out,
               xn_all, recv, d_recv, dy_rows, d_tok, gate_send, up_buf, lin_buf, down_buf, codes_buf, gates_buf,
               w_sem, x_send, x_recv, p_send, p_recv, own_sem, row_sem, b_send, b_recv, g_send, g_recv):
    z = lax.axis_index('dp')
    ep = lax.axis_index('ep')
    local_exp = up_ref.shape[0]
    plane = xn_all.shape[0]
    width = xn_ref.shape[1]
    first = pl.multiple_of(ep * local_exp, local_exp)
    bits = (lax.rem(ep, 2), lax.rem(ep // 2, 2), ep // 4)

    def flipped(d):
        flags = (lax.rem(d, 2), lax.rem(d // 2, 2), d // 4)
        both = [b + f - 2 * b * f for b, f in zip(bits, flags)]
        return both[0] + 2 * both[1] + 4 * both[2]

    def copy(src, dst, s_sem, r_sem, dev):
        return pltpu.make_async_remote_copy(src_ref=src, dst_ref=dst, send_sem=s_sem, recv_sem=r_sem,
                                            device_id=(z, dev), device_id_type=MESH)

    def weights(e, slot):
        return [pltpu.make_async_copy(src.at[e], dst.at[slot], w_sem.at[i, slot])
                for i, (src, dst) in enumerate(((up_ref, up_buf), (lin_ref, lin_buf), (down_ref, down_buf)))]

    for i in (1, 2, 3):
        copy(xn_ref, xn_all.at[ep], x_send.at[i], x_recv.at[i], flipped(2 * i)).start()
    copy(xn_ref, xn_all.at[ep], p_send.at[0], p_recv.at[0], flipped(1)).start()
    for c in weights(0, 0):
        c.start()
    xn_all[ep] = xn_ref[...]
    router = router_ref[...]

    def pair(i, _):
        near = flipped(2 * i)
        other = flipped(2 * i + 1)

        @pl.when(i > 0)
        def _():
            copy(xn_ref, xn_all.at[near], x_send.at[i], x_recv.at[i], near).wait_recv()
            copy(xn_all.at[near], xn_all.at[near], p_send.at[i], p_recv.at[i], flipped(1)).start()

        copy(xn_ref, xn_all.at[other], p_send.at[i], p_recv.at[i], flipped(1)).wait_recv()
        for j, src in enumerate((near, other)):
            rows, dy, gate_slot = slot_rows(xn_all[src], dyc_ref[src], router, first, local_exp, cap, codes_buf.at[j], gates_buf.at[j])
            at = pl.ds(pl.multiple_of(src * cap, cap), cap)
            recv[:, at, :] = rows.reshape(local_exp, cap, width)
            dy_rows[:, at, :] = dy.astype(BF16).reshape(local_exp, cap, width)
            d_recv[:, at, :] = (gate_slot * dy).astype(BF16).reshape(local_exp, cap, width)
        return 0

    lax.fori_loop(0, plane // 2, pair, 0)

    keep = [pltpu.make_async_copy(src, dst.at[:, pl.ds(0, plane * cap), :], row_sem.at[i])
            for i, (src, dst) in enumerate(((recv, recv_out), (d_recv, d_recv_out)))]
    for c in keep:
        c.start()

    def home(d, e):
        dev = flipped(d)
        src = d_tok.at[e, pl.ds(pl.multiple_of(dev * cap, cap), cap), :]
        return copy(src, back_ref.at[first + e], b_send.at[d, e], b_recv.at[d, e], dev)

    def stay(e):
        return pltpu.make_async_copy(d_tok.at[e, pl.ds(pl.multiple_of(ep * cap, cap), cap), :], back_ref.at[first + e], own_sem.at[e])

    def expert(e, _):
        slot = lax.rem(e, 2)

        @pl.when(e + 1 < local_exp)
        def _():
            for c in weights(e + 1, 1 - slot):
                c.start()

        for c in weights(e, slot):
            c.wait()
        up, lin, down = up_buf[slot], lin_buf[slot], down_buf[slot]
        act, d_u, d_v = hidden_grads(recv[e], d_recv[e], up, lin, down)
        d_tok[e] = (dot_nt(d_u, up) + dot_nt(d_v, lin)).astype(BF16)
        y = dot_nn(act, down).astype(BF16).astype(F32)
        d_gate = jnp.sum(dy_rows[e].astype(F32) * y, axis=-1, keepdims=True)
        lane = lax.broadcasted_iota(jnp.int32, (plane, cap, 128), 2)
        row = lax.broadcasted_iota(jnp.int32, (plane, cap, 128), 1)
        wide = jnp.broadcast_to(d_gate, (plane * cap, 128)).reshape(plane, cap, 128)
        gate_send[:, pl.ds(e, 1), :] = jnp.sum(jnp.where(lane == row, wide, 0.0), axis=1, keepdims=True)
        for d in (6, 7, 2, 3, 4, 5, 1):
            home(d, e).start()
        stay(e).start()
        return 0

    lax.fori_loop(0, local_exp, expert, 0)

    for c in keep:
        c.wait()

    def gate_home(d):
        dev = flipped(d)
        return copy(gate_send.at[dev], gate_back_ref.at[ep], g_send.at[d], g_recv.at[d], dev)

    for d in range(1, plane):
        gate_home(d).start()
    gate_back_ref[ep] = gate_send[ep]

    def drain(e, _):
        for d in range(1, plane):
            src = d_tok.at[0, pl.ds(0, cap), :]
            copy(src, back_ref.at[flipped(d) * local_exp + e], b_send.at[d, e], b_recv.at[d, e], flipped(d)).wait_recv()
            home(d, e).wait_send()
        stay(e).wait()
        return 0

    lax.fori_loop(0, local_exp, drain, 0)
    for d in range(1, plane):
        copy(gate_send.at[0], gate_back_ref.at[flipped(d)], g_send.at[d], g_recv.at[d], flipped(d)).wait_recv()
        gate_home(d).wait_send()
    for i in (1, 2, 3):
        copy(xn_ref, xn_all.at[ep], x_send.at[i], x_recv.at[i], flipped(2 * i)).wait_send()
        copy(xn_all.at[flipped(2 * i)], xn_all.at[flipped(2 * i)], p_send.at[i], p_recv.at[i], flipped(1)).wait_send()
    copy(xn_ref, xn_all.at[ep], p_send.at[0], p_recv.at[0], flipped(1)).wait_send()


def moe_backward(xn, dyc_plane, router_t, w_up, w_lin, w_down, cap, planes):
    plane, tokens = dyc_plane.shape[:2]
    local_exp, width, hid = w_up.shape
    experts = router_t.shape[0]
    rows = pltpu.VMEM((local_exp, plane * cap, width), BF16)
    vmem = pl.BlockSpec(memory_space=pltpu.VMEM)
    any_spec = pl.BlockSpec(memory_space=pl.ANY)
    dma = pltpu.SemaphoreType.DMA
    return pl.pallas_call(
        functools.partial(moe_kernel, cap),
        out_shape=(jax.ShapeDtypeStruct((experts, cap, width), BF16), jax.ShapeDtypeStruct((plane, local_exp, 128), F32),
                   jax.ShapeDtypeStruct((local_exp, planes * plane * cap, width), BF16),
                   jax.ShapeDtypeStruct((local_exp, planes * plane * cap, width), BF16)),
        in_specs=[vmem, vmem, vmem, any_spec, any_spec, any_spec],
        out_specs=(any_spec, vmem, any_spec, any_spec),
        scratch_shapes=[
            pltpu.VMEM((plane, tokens, width), BF16), rows, rows, rows, rows, pltpu.VMEM((plane, local_exp, 128), F32),
            pltpu.VMEM((2, width, hid), BF16), pltpu.VMEM((2, width, hid), BF16), pltpu.VMEM((2, hid, width), BF16),
            pltpu.VMEM((2, experts, tokens), F32), pltpu.VMEM((2, experts, tokens), F32),
            dma((3, 2)), dma((4,)), dma((4,)), dma((4,)), dma((4,)), dma((local_exp,)), dma((2,)),
            dma((plane, local_exp)), dma((plane, local_exp)), dma((plane,)), dma((plane,)),
        ],
        compiler_params=pltpu.CompilerParams(has_side_effects=True, vmem_limit_bytes=60 << 20),
        cost_estimate=pl.CostEstimate(flops=60 * 10**9, bytes_accessed=64 << 20, transcendentals=0),
        name='moe_backward',
    )(xn, dyc_plane, router_t, w_up, w_lin, w_down)


def weight_kernel(recv_ref, d_recv_ref, up_ref, lin_ref, down_ref, *rest):
    g_up_ref, g_lin_ref, g_down_ref, act_buf, du_buf, dv_buf = rest[-6:]
    total = recv_ref.shape[1]
    block = 256

    @pl.loop(0, total // block)
    def _(i):
        rows = pl.ds(pl.multiple_of(i * block, block), block)
        act, d_u, d_v = hidden_grads(recv_ref[0, rows, :], d_recv_ref[0, rows, :], up_ref[0], lin_ref[0], down_ref[0])
        act_buf[rows, :] = act
        du_buf[rows, :] = d_u
        dv_buf[rows, :] = d_v

    width = recv_ref.shape[2]
    cols = 512

    @pl.loop(0, width // cols)
    def _(i):
        c = pl.ds(pl.multiple_of(i * cols, cols), cols)
        g_up_ref[0, c, :] = dot_tn(recv_ref[0, :, c], du_buf[...])
        g_lin_ref[0, c, :] = dot_tn(recv_ref[0, :, c], dv_buf[...])
        g_down_ref[0, :, c] = dot_tn(act_buf[...], d_recv_ref[0, :, c])


def weight_grads(recv, d_recv, w_up, w_lin, w_down, first, count, grads=()):
    _, total, width = recv.shape
    hid = w_up.shape[2]
    rows = pl.BlockSpec((1, total, width), lambda e: (first + e, 0, 0))
    wide = pl.BlockSpec((1, width, hid), lambda e: (first + e, 0, 0))
    tall = pl.BlockSpec((1, hid, width), lambda e: (first + e, 0, 0))
    f32 = lambda arr: jax.ShapeDtypeStruct(arr.shape, F32)
    return pl.pallas_call(
        weight_kernel,
        grid=(count,),
        out_shape=(f32(w_up), f32(w_lin), f32(w_down)),
        in_specs=[rows, rows, wide, wide, tall] + [pl.BlockSpec(memory_space=pl.ANY)] * len(grads),
        out_specs=(wide, wide, tall),
        scratch_shapes=[pltpu.VMEM((total, hid), BF16)] * 3,
        input_output_aliases={5 + i: i for i in range(len(grads))},
        compiler_params=pltpu.CompilerParams(vmem_limit_bytes=60 << 20),
        cost_estimate=pl.CostEstimate(flops=12 * count * total * width * hid, transcendentals=0, bytes_accessed=count * (20 << 20)),
        name='weight_grads',
    )(recv, d_recv, w_up, w_lin, w_down, *grads)


def solution(mesh):
    tok_spec = P(('dp', 'ep'))
    exp_spec = P('ep')
    rep_spec = P()
    world = ('dp', 'ep')

    def local(x_in, dy_in, route_idx, gain_attn, w_qkv, w_o, gain_ffn, w_router, w_up, w_lin, w_down):
        num_seqs, seq_len, width = x_in.shape
        tokens = num_seqs * seq_len
        top = route_idx.shape[-1]
        experts = w_router.shape[1]
        local_exp = w_up.shape[0]
        cap = ((tokens * top * 5) // (experts * 4) + 7) // 8 * 8
        ep_size = mesh.shape['ep']

        codes = slot_codes(route_idx.reshape(tokens, top), experts, cap)
        dy_own = dy_in.reshape(tokens, width)
        lanes = jnp.zeros((tokens, HEAD - experts), BF16)
        dyc_own = jnp.concatenate([dy_own, codes.T, lanes], axis=1)
        dyc_plane = lax.all_gather(dyc_own, 'ep')
        dyc_all = lax.all_gather(dyc_own, world)
        router_t = w_router.T
        planes = mesh.shape['dp']
        my_z = lax.axis_index('dp')

        def spread(act):
            halves = jnp.moveaxis(act.reshape(tokens, 2, width // 2), 1, 0)
            send = jnp.broadcast_to(halves[None], (ep_size // 2, 2, tokens, width // 2)).reshape(ep_size, tokens, width // 2)
            return lax.all_to_all(send, 'ep', 0, 0).reshape(ep_size * tokens, width // 2)

        x_f = x_in.astype(F32)
        xn_one, norm_one_pull = jax.vjp(rms_norm, x_f, gain_attn.astype(F32))
        acts_xn = spread(xn_one)
        qkv_all = mm('bsd,de->bse', xn_one, w_qkv).astype(BF16)
        attn_out, attn_pull = jax.vjp(attn_core, qkv_all)
        attn_proj = mm('bsd,de->bse', attn_out, w_o)
        hidden = (x_f + attn_proj).astype(BF16).astype(F32).reshape(tokens, width)
        xn_two, norm_two_pull = jax.vjp(rms_norm, hidden, gain_ffn.astype(F32))

        xn_all = lax.all_gather(xn_two, world)
        d_back, gate_back, recv, d_recv = moe_backward(after(xn_two, acts_xn), dyc_plane, router_t, w_up, w_lin, w_down, cap, planes)
        acts_ao = spread(after(attn_out, gate_back))
        d_gate_back = gate_back[:, :, :cap].reshape(experts, cap)

        select_own = one_hot(codes, cap)
        d_moe_in = mm('ect,ecd->td', select_own, d_back)
        prob, mask, gates, total = gates_of(xn_two, codes, w_router)
        d_gates = jnp.sum(select_own.astype(F32) * d_gate_back[:, :, None], axis=1)
        d_picked = (d_gates - jnp.sum(d_gates * gates, axis=0, keepdims=True)) / total * mask
        d_logits = (prob * (d_picked - jnp.sum(prob * d_picked, axis=0, keepdims=True))).astype(BF16)
        d_xn_two = (d_moe_in + mm('et,de->td', d_logits, w_router)).astype(BF16)
        d_logits_all = lax.all_gather(d_logits.T, world)
        d_hidden, grad_gain_ffn = norm_two_pull(d_xn_two)
        d_resid = (d_hidden + dy_own.astype(F32)).astype(BF16).reshape(num_seqs, seq_len, width)
        d_attn_out = mm('bse,de->bsd', d_resid, w_o).astype(BF16)
        d_qkv = attn_pull(d_attn_out)[0]
        d_xn_one = mm('bse,de->bsd', d_qkv, w_qkv).astype(BF16)
        d_x_norm, grad_gain_attn = norm_one_pull(d_xn_one)
        dx_out = (d_x_norm + d_resid.astype(F32)).astype(BF16)
        quarters = lambda arr: jnp.moveaxis(arr.reshape(tokens, 4, -1), 1, 0)
        dsend = jnp.concatenate([quarters(d_qkv), quarters(d_resid)], axis=2)
        gains = jnp.concatenate([grad_gain_attn, grad_gain_ffn]).reshape(-1, 128)
        low, high, gains = dense_sums(acts_xn, acts_ao, dsend, gains)
        grad_gain_attn, grad_gain_ffn = gains.reshape(2, width)

        flip = lambda arr, bit: lax.ppermute(arr, 'ep', [(e, e ^ bit) for e in range(ep_size)])
        low_x, high_y = flip(low, 2), flip(high, 4)
        low_y, high_x = flip(low, 4), flip(high, 2)
        low_xy, high_xy = flip(low_x, 4), flip(high_y, 2)
        pieces = [low, high, low_x, high_x, low_y, high_y, low_xy, high_xy]
        swapped = [flip(arr, 1) for arr in pieces[:6]]
        swapped += [flip(arr, 1) for arr in pieces[6:]]
        pieces = [arr for i in range(4) for arr in (pieces[2 * i], pieces[2 * i + 1], swapped[2 * i], swapped[2 * i + 1])]

        xn_late, dyc_late, d_logits_late = lax.optimization_barrier((xn_all, dyc_all, d_logits_all, gains))[:3]
        grad_router = mm('ntd,nte->de', xn_late, d_logits_late)
        xn_late = xn_late.reshape(planes, ep_size, tokens, width)
        dyc_late = dyc_late.reshape(planes, ep_size, tokens, -1)
        recv, d_recv = dispatch_rows(my_z.reshape(1), xn_late, dyc_late, router_t, recv, d_recv, cap)
        grads = weight_grads(recv, d_recv, w_up, w_lin, w_down, 0, local_exp // 2)
        grad_up, grad_lin, grad_down = weight_grads(recv, d_recv, w_up, w_lin, w_down, local_exp // 2, local_exp // 2, grads)
        grad_wqkv, grad_wo = assemble(pieces)
        return (dx_out, grad_gain_attn, grad_wqkv, grad_wo, grad_gain_ffn, grad_router, grad_up, grad_lin, grad_down)

    in_specs = (tok_spec, tok_spec, tok_spec, rep_spec, rep_spec, rep_spec, rep_spec, rep_spec, exp_spec, exp_spec, exp_spec)
    out_specs = (tok_spec, rep_spec, rep_spec, rep_spec, rep_spec, rep_spec, exp_spec, exp_spec, exp_spec)

    return jax.shard_map(local, mesh=mesh, in_specs=in_specs, out_specs=out_specs, check_vma=False)
```

```python
import functools

import jax
import jax.numpy as jnp
from jax import lax
from jax.experimental import pallas as pl
from jax.experimental.pallas import tpu as pltpu
from jax.sharding import PartitionSpec as P


EPS = 1e-6
HEAD = 128
DROPPED = 64.0
UNCHOSEN = 128.0
F32 = jnp.float32
BF16 = jnp.bfloat16


def mm(spec, a, b):
    return jnp.einsum(spec, a, b, preferred_element_type=F32)


def rms_norm(values, gain):
    scale = lax.rsqrt(jnp.mean(values * values, axis=-1, keepdims=True) + EPS)
    return (values * scale * gain).astype(BF16)


def attn_core(qkv_rows):
    num_seqs, seq_len, width = qkv_rows.shape
    heads = width // (3 * HEAD)
    split = qkv_rows.reshape(num_seqs, seq_len, 3, heads, HEAD)
    scores = mm('bqhc,bkhc->bhqk', split[:, :, 0], split[:, :, 1]) * (HEAD ** -0.5)
    rows = lax.broadcasted_iota(jnp.int32, (seq_len, seq_len), 0)
    cols = lax.broadcasted_iota(jnp.int32, (seq_len, seq_len), 1)
    scores = jnp.where(rows >= cols, scores, -1e30)
    prob_rows = jax.nn.softmax(scores, axis=-1).astype(BF16)
    mixed = mm('bhqk,bkhc->bqhc', prob_rows, split[:, :, 2])
    return mixed.astype(BF16).reshape(num_seqs, seq_len, heads * HEAD)


def slot_codes(idx_rows, experts, cap):
    tokens = idx_rows.shape[0]
    chosen = jnp.any(idx_rows[:, :, None] == jnp.arange(experts, dtype=jnp.int32), axis=1).astype(BF16)
    rows = lax.broadcasted_iota(jnp.int32, (tokens, tokens), 0)
    cols = lax.broadcasted_iota(jnp.int32, (tokens, tokens), 1)
    prior = mm('se,st->et', chosen, (rows < cols).astype(BF16))
    taken = mm('se,st->et', chosen, (rows == cols).astype(BF16))
    return jnp.where(taken > 0.5, jnp.where(prior < cap, prior, DROPPED), UNCHOSEN).astype(BF16)


def one_hot(codes, cap):
    slots = lax.broadcasted_iota(jnp.int32, codes.shape[:-1] + (cap, codes.shape[-1]), codes.ndim - 1)
    return (codes[..., None, :].astype(F32) == slots.astype(F32)).astype(BF16)


def gates_of(xn, codes, w_router):
    logits = mm('...td,de->...et', xn, w_router)
    prob = jax.nn.softmax(logits, axis=-2)
    mask = (codes.astype(F32) < UNCHOSEN - 1.0).astype(F32)
    picked = prob * mask
    total = jnp.sum(picked, axis=-2, keepdims=True)
    return prob, mask, picked / total, total


def after(value, *deps):
    return lax.optimization_barrier((value,) + deps)[0]


HALF = 768
CHUNK = 128
STEPS = HALF // CHUNK
MESH = pl.DeviceIdType.MESH


def dot_tn(a, b):
    return lax.dot_general(a, b, (((0,), (0,)), ((), ())), preferred_element_type=jnp.float32)


def dense_kernel(acts_ref, dsend_ref, gains_ref, router_ref, low_ref, high_ref, gains_out_ref, router_out_ref,
                 dall, part, z_in, total, gain_buf, router_buf,
                 d_send, d_recv, dp_send, dp_recv, z_send, z_recv, own_sem, g_send, g_recv, r_send, r_recv, s_send, s_recv):
    z = lax.axis_index('dp')
    ep = lax.axis_index('ep')
    core = lax.rem(ep, 2)
    quarter = ep // 2
    width = dsend_ref.shape[2]
    split = width * 3 // 4
    tokens = dsend_ref.shape[1]
    partner = ep + 1 - 2 * core
    bit_x = lax.rem(quarter, 2)
    bit_y = quarter // 2
    flip = lambda bx, by: 2 * ((bit_x + bx - 2 * bit_x * bx) + 2 * (bit_y + by - 2 * bit_y * by)) + core
    x_dev, y_dev, xy_dev = flip(1, 0), flip(0, 1), flip(1, 1)
    inner = jnp.logical_or(z == 1, z == 2)
    z_mate = jnp.where(z == 0, 1, jnp.where(z == 1, 0, jnp.where(z == 2, 3, 2)))
    z_cross = 3 - z

    def copy(src, dst, s_sem, r_sem, dp, e):
        return pltpu.make_async_remote_copy(src_ref=src, dst_ref=dst, send_sem=s_sem, recv_sem=r_sem,
                                            device_id=(dp, e), device_id_type=MESH)

    rows_of = lambda e: pl.ds(pl.multiple_of(e * tokens, tokens), tokens)
    far = (x_dev, y_dev, xy_dev)
    for i, dev in enumerate(far):
        copy(dsend_ref.at[dev // 2], dall.at[rows_of(ep)], d_send.at[i], d_recv.at[i], z, dev).start()
    copy(dsend_ref.at[quarter], dall.at[rows_of(ep)], dp_send.at[3], dp_recv.at[3], z, partner).start()

    world = router_ref.shape[0]
    me = z * 8 + ep

    def push(pick, buf, s_sem, r_sem, d, target):
        return copy(pick(target), buf.at[me], s_sem.at[d], r_sem.at[d], target // 8, lax.rem(target, 8))

    def push_all(*args):
        def body(d, _):
            push(*args, d, lax.rem(me + d, world)).start()
            return 0

        lax.fori_loop(1, world, body, 0)

    def wait_all(pick, buf, s_sem, r_sem):
        def body(d, _):
            push(pick, buf, s_sem, r_sem, d, lax.rem(me + d, world)).wait()
            return 0

        lax.fori_loop(1, world, body, 0)

    def device_sum(buf):
        return lax.fori_loop(0, world, lambda s, acc: acc + buf[s], jnp.zeros(buf.shape[1:], jnp.float32))

    gain_push = (lambda t: gains_ref, gain_buf, g_send, g_recv)
    share_push = (lambda t: router_ref.at[t], router_buf, r_send, r_recv)
    total_push = (lambda t: router_out_ref.at[me], router_out_ref, s_send, s_recv)
    push_all(*gain_push)
    push_all(*share_push)

    dall[rows_of(ep), :] = dsend_ref[quarter]
    for i, dev in enumerate(far):
        copy(dsend_ref.at[dev // 2], dall.at[rows_of(dev)], d_send.at[i], d_recv.at[i], z, dev).wait_recv()
        copy(dall.at[rows_of(dev)], dall.at[rows_of(dev)], dp_send.at[i], dp_recv.at[i], z, partner).start()
    for i, dev in enumerate(far + (ep,)):
        other = dev + 1 - 2 * core
        copy(dsend_ref.at[0], dall.at[rows_of(other)], dp_send.at[i], dp_recv.at[i], z, partner).wait_recv()

    up_copy = lambda k: copy(part.at[k], z_in.at[k], z_send.at[0, k], z_recv.at[0, k], z_mate, ep)
    cross_copy = lambda k: copy(part.at[k], total.at[k], z_send.at[1, k], z_recv.at[1, k], z_cross, ep)
    down_copy = lambda k: copy(total.at[k], total.at[k], z_send.at[2, k], z_recv.at[2, k], z_mate, ep)

    def own_copy(k):
        ref = low_ref if k < STEPS // 2 else high_ref
        return pltpu.make_async_copy(total.at[k], ref.at[pl.ds(k % (STEPS // 2) * CHUNK, CHUNK), :], own_sem.at[k])

    for i in range(STEPS + 3):
        k = i
        if k < STEPS:
            cols = slice(k * CHUNK, (k + 1) * CHUNK)
            cols_o = slice(HALF + k * CHUNK, HALF + (k + 1) * CHUNK)
            part[k, :, :split] = dot_tn(acts_ref[:, cols], dall[:, :split])
            part[k, :, split:] = dot_tn(acts_ref[:, cols_o], dall[:, split:])
        if i == 3:
            wait_all(*share_push)
            router_buf[me] = router_ref[me]
            router_out_ref[me] = device_sum(router_buf)
        if i == 4:
            push_all(*total_push)
        a = i - 1
        t = i - 2

        @pl.when(inner)
        def _():
            if 0 <= a < STEPS:
                up_copy(a).wait_recv()
                part[a] = part[a] + z_in[a]
            if 0 <= t < STEPS:
                cross_copy(t).wait_recv()
                total[t] = part[t] + total[t]
            if 0 <= a < STEPS:
                cross_copy(a).start()
            if 0 <= t < STEPS:
                down_copy(t).start()
                own_copy(t).start()

        @pl.when(jnp.logical_not(inner))
        def _():
            if k < STEPS:
                up_copy(k).start()
            if 0 <= i - 3 < STEPS:
                down_copy(i - 3).wait_recv()
                own_copy(i - 3).start()

    for k in range(STEPS):
        own_copy(k).wait()

    @pl.when(inner)
    def _():
        for k in range(STEPS):
            cross_copy(k).wait_send()
            down_copy(k).wait_send()

    @pl.when(jnp.logical_not(inner))
    def _():
        for k in range(STEPS):
            up_copy(k).wait_send()

    for i, dev in enumerate(far):
        copy(dsend_ref.at[dev // 2], dall.at[rows_of(ep)], d_send.at[i], d_recv.at[i], z, dev).wait_send()
        copy(dall.at[rows_of(dev)], dall.at[rows_of(dev)], dp_send.at[i], dp_recv.at[i], z, partner).wait_send()
    copy(dsend_ref.at[quarter], dall.at[rows_of(ep)], dp_send.at[3], dp_recv.at[3], z, partner).wait_send()

    wait_all(*gain_push)
    gain_buf[me] = gains_ref[...]
    gains_out_ref[...] = device_sum(gain_buf)
    wait_all(*total_push)


def dense_sums(acts, dsend, gains, router):
    rows, width = acts.shape[0], dsend.shape[2]
    any_spec = pl.BlockSpec(memory_space=pl.ANY)
    vmem = pl.BlockSpec(memory_space=pltpu.VMEM)
    dma = pltpu.SemaphoreType.DMA
    f32 = lambda *shape: jax.ShapeDtypeStruct(shape, jnp.float32)
    world = router.shape[0]
    return pl.pallas_call(
        dense_kernel,
        out_shape=(f32(HALF // 2, width), f32(HALF // 2, width), f32(*gains.shape), f32(*router.shape)),
        in_specs=[vmem, vmem, vmem, vmem],
        out_specs=(any_spec, any_spec, vmem, vmem),
        scratch_shapes=[
            pltpu.VMEM((rows, width), jnp.bfloat16),
            pltpu.VMEM((STEPS, CHUNK, width), jnp.float32),
            pltpu.VMEM((STEPS, CHUNK, width), jnp.float32),
            pltpu.VMEM((STEPS, CHUNK, width), jnp.float32),
            pltpu.VMEM((world,) + gains.shape, jnp.float32),
            pltpu.VMEM(router.shape, jnp.float32),
            dma((3,)), dma((3,)), dma((4,)), dma((4,)), dma((3, STEPS)), dma((3, STEPS)), dma((STEPS,)),
            dma((world,)), dma((world,)), dma((world,)), dma((world,)), dma((world,)), dma((world,)),
        ],
        compiler_params=pltpu.CompilerParams(has_side_effects=True, vmem_limit_bytes=48 << 20),
        cost_estimate=pl.CostEstimate(flops=100 * 10**9, bytes_accessed=40 << 20, transcendentals=0),
        name='dense_sums',
    )(acts, dsend, gains, router)


def assemble_kernel(*refs):
    pieces, (qkv_ref, wo_ref, buf, in_sem, out_sem) = refs[:16], refs[16:]
    ep = lax.axis_index('ep')
    bits = (lax.rem(ep, 2), lax.rem(ep // 2, 2), ep // 4)
    size = HALF // 2
    width = buf.shape[2]
    split = width * 3 // 4

    def load(n):
        return pltpu.make_async_copy(pieces[n], buf.at[n % 4], in_sem.at[n % 4])

    def stores(n):
        flips = (n // 2 % 2, n // 4 % 2, n // 8)
        core, bx, by = [b + f - 2 * b * f for b, f in zip(bits, flips)]
        rows = pl.ds(pl.multiple_of(core * HALF + n % 2 * size, size), size)
        q = bx + 2 * by
        return [pltpu.make_async_copy(buf.at[n % 4, :, pl.ds(lo, cols)],
                                      ref.at[rows, pl.ds(pl.multiple_of(q * cols, 128), cols)], out_sem.at[n % 4, i])
                for i, (ref, lo, cols) in enumerate(((qkv_ref, 0, split), (wo_ref, split, width - split)))]

    for n in range(16 + 2):
        if n < 16:
            if n >= 4:
                for c in stores(n - 4):
                    c.wait()
            load(n).start()
        if n >= 2:
            load(n - 2).wait()
            for c in stores(n - 2):
                c.start()
    for n in range(12, 16):
        for c in stores(n):
            c.wait()


def assemble(pieces):
    width = pieces[0].shape[1]
    any_spec = pl.BlockSpec(memory_space=pl.ANY)
    return pl.pallas_call(
        assemble_kernel,
        out_shape=(jax.ShapeDtypeStruct((2 * HALF, 3 * width), F32), jax.ShapeDtypeStruct((2 * HALF, width), F32)),
        in_specs=[any_spec] * 16,
        out_specs=(any_spec, any_spec),
        scratch_shapes=[pltpu.VMEM((4, HALF // 2, width), F32), pltpu.SemaphoreType.DMA((4,)), pltpu.SemaphoreType.DMA((4, 2))],
        compiler_params=pltpu.CompilerParams(vmem_limit_bytes=24 << 20),
        cost_estimate=pl.CostEstimate(flops=20 * 10**9, bytes_accessed=80 << 20, transcendentals=0),
        name='assemble',
    )(*pieces)


def dot_nn(a, b):
    return lax.dot_general(a, b, (((1,), (0,)), ((), ())), preferred_element_type=jnp.float32)


def dot_nt(a, b):
    return lax.dot_general(a, b, (((1,), (1,)), ((), ())), preferred_element_type=jnp.float32)


def slot_select(codes_t, gates, first, local_exp, cap, codes_buf, gates_buf):
    tokens = codes_t.shape[1]
    codes_buf[...] = codes_t
    gates_buf[...] = gates
    my_codes = codes_buf[pl.ds(first, local_exp), :]
    my_gates = gates_buf[pl.ds(first, local_exp), :]
    slots = lax.broadcasted_iota(jnp.int32, (local_exp, cap, tokens), 1).astype(F32)
    select = jnp.where(my_codes[:, None, :] == slots, 1.0, 0.0)
    gate_slot = jnp.sum(select * my_gates[:, None, :], axis=-1, keepdims=True).reshape(local_exp * cap, 1)
    return select.reshape(local_exp * cap, tokens).astype(BF16), gate_slot


def slot_rows(xn, dyc, router, first, local_exp, cap, codes_buf, gates_buf):
    experts = router.shape[0]
    width = xn.shape[1]
    codes = dyc[:, width:].astype(F32).T[:experts]
    logits = dot_nt(router, xn)
    prob = jnp.exp(logits - jnp.max(logits, axis=0, keepdims=True))
    prob = prob / jnp.sum(prob, axis=0, keepdims=True)
    picked = jnp.where(codes < UNCHOSEN - 1.0, prob, 0.0)
    gates = picked / jnp.sum(picked, axis=0, keepdims=True)
    select, gate_slot = slot_select(codes, gates, first, local_exp, cap, codes_buf, gates_buf)
    return dot_nn(select, xn).astype(BF16), dot_nn(select, dyc[:, :width]), gate_slot


def dispatch_kernel(local_exp, cap, rows_ref, router_ref, recv_in, d_recv_in, recv_ref, d_recv_ref, codes_buf, gates_buf):
    first = pl.multiple_of(lax.axis_index('ep') * local_exp, local_exp)
    router = router_ref[...]
    width = router.shape[1]
    for i in range(rows_ref.shape[0]):
        recv, dy_rows, gate_slot = slot_rows(rows_ref[i, :, :width], rows_ref[i, :, width:], router, first, local_exp, cap,
                                             codes_buf.at[i], gates_buf.at[i])
        at = slice(i * cap, (i + 1) * cap)
        recv_ref[:, at, :] = recv.reshape(local_exp, cap, width)
        d_recv_ref[:, at, :] = (gate_slot * dy_rows).astype(BF16).reshape(local_exp, cap, width)


def dispatch_rows(rows, router_t, recv, d_recv, skip, cap):
    sources, tokens, lanes = rows.shape
    local_exp, _, width = recv.shape
    experts = router_t.shape[0]
    step = 4
    any_spec = pl.BlockSpec(memory_space=pl.ANY)
    out_spec = pl.BlockSpec((local_exp, step * cap, width), lambda s: (0, skip // (step * cap) + s, 0))
    same = lambda arr: jax.ShapeDtypeStruct(arr.shape, arr.dtype)
    return pl.pallas_call(
        functools.partial(dispatch_kernel, local_exp, cap),
        grid=(sources // step,),
        in_specs=[pl.BlockSpec((step, tokens, lanes), lambda s: (s, 0, 0)), pl.BlockSpec(router_t.shape, lambda s: (0, 0)), any_spec, any_spec],
        out_specs=(out_spec, out_spec),
        scratch_shapes=[pltpu.VMEM((step, experts, tokens), F32), pltpu.VMEM((step, experts, tokens), F32)],
        out_shape=(same(recv), same(d_recv)),
        input_output_aliases={2: 0, 3: 1},
        compiler_params=pltpu.CompilerParams(vmem_limit_bytes=56 << 20),
        cost_estimate=pl.CostEstimate(flops=sources * 4 * local_exp * cap * tokens * width, transcendentals=0,
                                      bytes_accessed=sources * tokens * width * 8),
        name='dispatch_rows',
    )(rows, router_t, recv, d_recv)


def hidden_grads(recv, d_recv, up, lin, down):
    u = dot_nn(recv, up).astype(BF16).astype(F32)
    v = dot_nn(recv, lin).astype(BF16).astype(F32)
    d_act = dot_nt(d_recv, down).astype(BF16).astype(F32)
    sig = jax.nn.sigmoid(u)
    act = u * sig
    d_u = d_act * v * (sig + act * (1.0 - sig))
    return (act * v).astype(BF16), d_u.astype(BF16), (d_act * act).astype(BF16)


def moe_kernel(cap, xn_ref, dyc_ref, router_ref, up_ref, lin_ref, down_ref, back_ref, gate_back_ref, recv_out, d_recv_out,
               xn_all, recv, d_recv, dy_rows, d_tok, gate_send, up_buf, lin_buf, down_buf, codes_buf, gates_buf,
               w_sem, x_send, x_recv, p_send, p_recv, own_sem, row_sem, b_send, b_recv, g_send, g_recv):
    z = lax.axis_index('dp')
    ep = lax.axis_index('ep')
    local_exp = up_ref.shape[0]
    plane = xn_all.shape[0]
    width = xn_ref.shape[1]
    first = pl.multiple_of(ep * local_exp, local_exp)
    bits = (lax.rem(ep, 2), lax.rem(ep // 2, 2), ep // 4)

    def flipped(d):
        flags = (lax.rem(d, 2), lax.rem(d // 2, 2), d // 4)
        both = [b + f - 2 * b * f for b, f in zip(bits, flags)]
        return both[0] + 2 * both[1] + 4 * both[2]

    def copy(src, dst, s_sem, r_sem, dev):
        return pltpu.make_async_remote_copy(src_ref=src, dst_ref=dst, send_sem=s_sem, recv_sem=r_sem,
                                            device_id=(z, dev), device_id_type=MESH)

    def weights(e, slot):
        return [pltpu.make_async_copy(src.at[e], dst.at[slot], w_sem.at[i, slot])
                for i, (src, dst) in enumerate(((up_ref, up_buf), (lin_ref, lin_buf), (down_ref, down_buf)))]

    for i in (1, 2, 3):
        copy(xn_ref, xn_all.at[ep], x_send.at[i], x_recv.at[i], flipped(2 * i)).start()
    copy(xn_ref, xn_all.at[ep], p_send.at[0], p_recv.at[0], flipped(1)).start()
    for c in weights(0, 0):
        c.start()
    xn_all[ep] = xn_ref[...]
    router = router_ref[...]

    def pair(i, _):
        near = flipped(2 * i)
        other = flipped(2 * i + 1)

        @pl.when(i > 0)
        def _():
            copy(xn_ref, xn_all.at[near], x_send.at[i], x_recv.at[i], near).wait_recv()
            copy(xn_all.at[near], xn_all.at[near], p_send.at[i], p_recv.at[i], flipped(1)).start()

        copy(xn_ref, xn_all.at[other], p_send.at[i], p_recv.at[i], flipped(1)).wait_recv()
        for j, src in enumerate((near, other)):
            rows, dy, gate_slot = slot_rows(xn_all[src], dyc_ref[src], router, first, local_exp, cap, codes_buf.at[j], gates_buf.at[j])
            at = pl.ds(pl.multiple_of(src * cap, cap), cap)
            recv[:, at, :] = rows.reshape(local_exp, cap, width)
            dy_rows[:, at, :] = dy.astype(BF16).reshape(local_exp, cap, width)
            d_recv[:, at, :] = (gate_slot * dy).astype(BF16).reshape(local_exp, cap, width)
        return 0

    lax.fori_loop(0, plane // 2, pair, 0)

    keep = [pltpu.make_async_copy(src, dst.at[:, pl.ds(0, plane * cap), :], row_sem.at[i])
            for i, (src, dst) in enumerate(((recv, recv_out), (d_recv, d_recv_out)))]
    for c in keep:
        c.start()

    def home(d, e):
        dev = flipped(d)
        src = d_tok.at[e, pl.ds(pl.multiple_of(dev * cap, cap), cap), :]
        return copy(src, back_ref.at[first + e], b_send.at[d, e], b_recv.at[d, e], dev)

    def stay(e):
        return pltpu.make_async_copy(d_tok.at[e, pl.ds(pl.multiple_of(ep * cap, cap), cap), :], back_ref.at[first + e], own_sem.at[e])

    def expert(e, _):
        slot = lax.rem(e, 2)

        @pl.when(e + 1 < local_exp)
        def _():
            for c in weights(e + 1, 1 - slot):
                c.start()

        for c in weights(e, slot):
            c.wait()
        up, lin, down = up_buf[slot], lin_buf[slot], down_buf[slot]
        act, d_u, d_v = hidden_grads(recv[e], d_recv[e], up, lin, down)
        d_tok[e] = (dot_nt(d_u, up) + dot_nt(d_v, lin)).astype(BF16)
        y = dot_nn(act, down).astype(BF16).astype(F32)
        d_gate = jnp.sum(dy_rows[e].astype(F32) * y, axis=-1, keepdims=True)
        lane = lax.broadcasted_iota(jnp.int32, (plane, cap, 128), 2)
        row = lax.broadcasted_iota(jnp.int32, (plane, cap, 128), 1)
        wide = jnp.broadcast_to(d_gate, (plane * cap, 128)).reshape(plane, cap, 128)
        gate_send[:, pl.ds(e, 1), :] = jnp.sum(jnp.where(lane == row, wide, 0.0), axis=1, keepdims=True)
        for d in (6, 7, 2, 3, 4, 5, 1):
            home(d, e).start()
        stay(e).start()
        return 0

    lax.fori_loop(0, local_exp, expert, 0)

    for c in keep:
        c.wait()

    def gate_home(d):
        dev = flipped(d)
        return copy(gate_send.at[dev], gate_back_ref.at[ep], g_send.at[d], g_recv.at[d], dev)

    for d in range(1, plane):
        gate_home(d).start()
    gate_back_ref[ep] = gate_send[ep]

    def drain(e, _):
        for d in range(1, plane):
            src = d_tok.at[0, pl.ds(0, cap), :]
            copy(src, back_ref.at[flipped(d) * local_exp + e], b_send.at[d, e], b_recv.at[d, e], flipped(d)).wait_recv()
            home(d, e).wait_send()
        stay(e).wait()
        return 0

    lax.fori_loop(0, local_exp, drain, 0)
    for d in range(1, plane):
        copy(gate_send.at[0], gate_back_ref.at[flipped(d)], g_send.at[d], g_recv.at[d], flipped(d)).wait_recv()
        gate_home(d).wait_send()
    for i in (1, 2, 3):
        copy(xn_ref, xn_all.at[ep], x_send.at[i], x_recv.at[i], flipped(2 * i)).wait_send()
        copy(xn_all.at[flipped(2 * i)], xn_all.at[flipped(2 * i)], p_send.at[i], p_recv.at[i], flipped(1)).wait_send()
    copy(xn_ref, xn_all.at[ep], p_send.at[0], p_recv.at[0], flipped(1)).wait_send()


def moe_backward(xn, dyc_plane, router_t, w_up, w_lin, w_down, cap, planes):
    plane, tokens = dyc_plane.shape[:2]
    local_exp, width, hid = w_up.shape
    experts = router_t.shape[0]
    rows = pltpu.VMEM((local_exp, plane * cap, width), BF16)
    vmem = pl.BlockSpec(memory_space=pltpu.VMEM)
    any_spec = pl.BlockSpec(memory_space=pl.ANY)
    dma = pltpu.SemaphoreType.DMA
    return pl.pallas_call(
        functools.partial(moe_kernel, cap),
        out_shape=(jax.ShapeDtypeStruct((experts, cap, width), BF16), jax.ShapeDtypeStruct((plane, local_exp, 128), F32),
                   jax.ShapeDtypeStruct((local_exp, planes * plane * cap, width), BF16),
                   jax.ShapeDtypeStruct((local_exp, planes * plane * cap, width), BF16)),
        in_specs=[vmem, vmem, vmem, any_spec, any_spec, any_spec],
        out_specs=(any_spec, vmem, any_spec, any_spec),
        scratch_shapes=[
            pltpu.VMEM((plane, tokens, width), BF16), rows, rows, rows, rows, pltpu.VMEM((plane, local_exp, 128), F32),
            pltpu.VMEM((2, width, hid), BF16), pltpu.VMEM((2, width, hid), BF16), pltpu.VMEM((2, hid, width), BF16),
            pltpu.VMEM((2, experts, tokens), F32), pltpu.VMEM((2, experts, tokens), F32),
            dma((3, 2)), dma((4,)), dma((4,)), dma((4,)), dma((4,)), dma((local_exp,)), dma((2,)),
            dma((plane, local_exp)), dma((plane, local_exp)), dma((plane,)), dma((plane,)),
        ],
        compiler_params=pltpu.CompilerParams(has_side_effects=True, vmem_limit_bytes=60 << 20),
        cost_estimate=pl.CostEstimate(flops=60 * 10**9, bytes_accessed=64 << 20, transcendentals=0),
        name='moe_backward',
    )(xn, dyc_plane, router_t, w_up, w_lin, w_down)


def weight_kernel(recv_ref, d_recv_ref, up_ref, lin_ref, down_ref, *rest):
    g_up_ref, g_lin_ref, g_down_ref, act_buf, du_buf, dv_buf = rest[-6:]
    total = recv_ref.shape[1]
    block = 256

    @pl.loop(0, total // block)
    def _(i):
        rows = pl.ds(pl.multiple_of(i * block, block), block)
        act, d_u, d_v = hidden_grads(recv_ref[0, rows, :], d_recv_ref[0, rows, :], up_ref[0], lin_ref[0], down_ref[0])
        act_buf[rows, :] = act
        du_buf[rows, :] = d_u
        dv_buf[rows, :] = d_v

    width = recv_ref.shape[2]
    cols = 512

    @pl.loop(0, width // cols)
    def _(i):
        c = pl.ds(pl.multiple_of(i * cols, cols), cols)
        g_up_ref[0, c, :] = dot_tn(recv_ref[0, :, c], du_buf[...])
        g_lin_ref[0, c, :] = dot_tn(recv_ref[0, :, c], dv_buf[...])
        g_down_ref[0, :, c] = dot_tn(act_buf[...], d_recv_ref[0, :, c])


def weight_grads(recv, d_recv, w_up, w_lin, w_down, first, count, grads=()):
    _, total, width = recv.shape
    hid = w_up.shape[2]
    rows = pl.BlockSpec((1, total, width), lambda e: (first + e, 0, 0))
    wide = pl.BlockSpec((1, width, hid), lambda e: (first + e, 0, 0))
    tall = pl.BlockSpec((1, hid, width), lambda e: (first + e, 0, 0))
    f32 = lambda arr: jax.ShapeDtypeStruct(arr.shape, F32)
    return pl.pallas_call(
        weight_kernel,
        grid=(count,),
        out_shape=(f32(w_up), f32(w_lin), f32(w_down)),
        in_specs=[rows, rows, wide, wide, tall] + [pl.BlockSpec(memory_space=pl.ANY)] * len(grads),
        out_specs=(wide, wide, tall),
        scratch_shapes=[pltpu.VMEM((total, hid), BF16)] * 3,
        input_output_aliases={5 + i: i for i in range(len(grads))},
        compiler_params=pltpu.CompilerParams(vmem_limit_bytes=60 << 20),
        cost_estimate=pl.CostEstimate(flops=12 * count * total * width * hid, transcendentals=0, bytes_accessed=count * (20 << 20)),
        name='weight_grads',
    )(recv, d_recv, w_up, w_lin, w_down, *grads)


def solution(mesh):
    tok_spec = P(('dp', 'ep'))
    exp_spec = P('ep')
    rep_spec = P()

    def local(x_in, dy_in, route_idx, gain_attn, w_qkv, w_o, gain_ffn, w_router, w_up, w_lin, w_down):
        num_seqs, seq_len, width = x_in.shape
        tokens = num_seqs * seq_len
        top = route_idx.shape[-1]
        experts = w_router.shape[1]
        local_exp = w_up.shape[0]
        cap = ((tokens * top * 5) // (experts * 4) + 7) // 8 * 8
        ep_size = mesh.shape['ep']

        codes = slot_codes(route_idx.reshape(tokens, top), experts, cap)
        dy_own = dy_in.reshape(tokens, width)
        lanes = jnp.zeros((tokens, HEAD - experts), BF16)
        dyc_own = jnp.concatenate([dy_own, codes.T, lanes], axis=1)
        dyc_plane = lax.all_gather(dyc_own, 'ep')
        router_t = w_router.T
        planes = mesh.shape['dp']

        x_f = x_in.astype(F32)
        xn_one, norm_one_pull = jax.vjp(rms_norm, x_f, gain_attn.astype(F32))
        qkv_all = mm('bsd,de->bse', xn_one, w_qkv).astype(BF16)
        attn_out, attn_pull = jax.vjp(attn_core, qkv_all)
        attn_proj = mm('bsd,de->bse', attn_out, w_o)
        hidden = (x_f + attn_proj).astype(BF16).astype(F32).reshape(tokens, width)
        xn_two, norm_two_pull = jax.vjp(rms_norm, hidden, gain_ffn.astype(F32))

        rows_own = jnp.concatenate([xn_two, dyc_own], axis=1)
        foreign = [lax.ppermute(rows_own, 'dp', [((z + r) % planes, z) for z in range(planes)]) for r in range(1, planes)]
        d_back, gate_back, recv, d_recv = moe_backward(xn_two, dyc_plane, router_t, w_up, w_lin, w_down, cap, planes)
        both = jnp.stack([xn_one.reshape(tokens, width), attn_out.reshape(tokens, width)], axis=1)
        halves = jnp.moveaxis(both.reshape(tokens, 2, 2, width // 2), 2, 0).reshape(1, 2, tokens, width)
        send = jnp.broadcast_to(after(halves, gate_back), (ep_size // 2, 2, tokens, width)).reshape(ep_size, tokens, width)
        acts = lax.all_to_all(send, 'ep', 0, 0).reshape(ep_size * tokens, width)
        d_gate_back = gate_back[:, :, :cap].reshape(experts, cap)

        select_own = one_hot(codes, cap)
        d_moe_in = mm('ect,ecd->td', select_own, d_back)
        prob, mask, gates, total = gates_of(xn_two, codes, w_router)
        d_gates = jnp.sum(select_own.astype(F32) * d_gate_back[:, :, None], axis=1)
        d_picked = (d_gates - jnp.sum(d_gates * gates, axis=0, keepdims=True)) / total * mask
        d_logits = (prob * (d_picked - jnp.sum(prob * d_picked, axis=0, keepdims=True))).astype(BF16)
        d_xn_two = (d_moe_in + mm('et,de->td', d_logits, w_router)).astype(BF16)
        grad_router = mm('td,et->de', xn_two, d_logits)
        d_hidden, grad_gain_ffn = norm_two_pull(d_xn_two)
        d_resid = (d_hidden + dy_own.astype(F32)).astype(BF16).reshape(num_seqs, seq_len, width)
        d_attn_out = mm('bse,de->bsd', d_resid, w_o).astype(BF16)
        d_qkv = attn_pull(d_attn_out)[0]
        foreign = lax.all_gather(after(jnp.stack(foreign), acts, d_qkv), 'ep')
        d_xn_one = mm('bse,de->bsd', d_qkv, w_qkv).astype(BF16)
        d_x_norm, grad_gain_attn = norm_one_pull(d_xn_one)
        dx_out = (d_x_norm + d_resid.astype(F32)).astype(BF16)
        quarters = lambda arr: jnp.moveaxis(arr.reshape(tokens, 4, -1), 1, 0)
        dsend = jnp.concatenate([quarters(d_qkv), quarters(d_resid)], axis=2)
        gains = jnp.concatenate([grad_gain_attn, grad_gain_ffn]).reshape(-1, 128)
        world_size = planes * ep_size
        low, high, gains, grad_router = dense_sums(acts, dsend, gains, grad_router.reshape(world_size, -1, 128))
        grad_router = grad_router.reshape(width, experts)
        grad_gain_attn, grad_gain_ffn = gains.reshape(2, width)

        flip = lambda arr, bit: lax.ppermute(arr, 'ep', [(e, e ^ bit) for e in range(ep_size)])
        low_x, high_y = flip(low, 2), flip(high, 4)
        low_y, high_x = flip(low, 4), flip(high, 2)
        low_xy, high_xy = flip(low_x, 4), flip(high_y, 2)
        pieces = [low, high, low_x, high_x, low_y, high_y, low_xy, high_xy]
        swapped = [flip(arr, 1) for arr in pieces[:6]]
        swapped += [flip(arr, 1) for arr in pieces[6:]]
        pieces = [arr for i in range(4) for arr in (pieces[2 * i], pieces[2 * i + 1], swapped[2 * i], swapped[2 * i + 1])]

        foreign = after(foreign, gains)
        recv, d_recv = dispatch_rows(foreign.reshape(-1, tokens, foreign.shape[-1]), router_t, recv, d_recv, ep_size * cap, cap)
        grads = weight_grads(recv, d_recv, w_up, w_lin, w_down, 0, local_exp // 2)
        grad_up, grad_lin, grad_down = weight_grads(recv, d_recv, w_up, w_lin, w_down, local_exp // 2, local_exp // 2, grads)
        grad_wqkv, grad_wo = assemble(pieces)
        return (dx_out, grad_gain_attn, grad_wqkv, grad_wo, grad_gain_ffn, grad_router, grad_up, grad_lin, grad_down)

    in_specs = (tok_spec, tok_spec, tok_spec, rep_spec, rep_spec, rep_spec, rep_spec, rep_spec, exp_spec, exp_spec, exp_spec)
    out_specs = (tok_spec, rep_spec, rep_spec, rep_spec, rep_spec, rep_spec, exp_spec, exp_spec, exp_spec)

    return jax.shard_map(local, mesh=mesh, in_specs=in_specs, out_specs=out_specs, check_vma=False)
```

```python
import functools

import jax
import jax.numpy as jnp
from jax import lax
from jax.experimental import pallas as pl
from jax.experimental.pallas import tpu as pltpu
from jax.sharding import PartitionSpec as P


EPS = 1e-6
HEAD = 128
DROPPED = 64.0
UNCHOSEN = 128.0
F32 = jnp.float32
BF16 = jnp.bfloat16


def mm(spec, a, b):
    return jnp.einsum(spec, a, b, preferred_element_type=F32)


def rms_norm(values, gain):
    scale = lax.rsqrt(jnp.mean(values * values, axis=-1, keepdims=True) + EPS)
    return (values * scale * gain).astype(BF16)


def attn_core(qkv_rows):
    num_seqs, seq_len, width = qkv_rows.shape
    heads = width // (3 * HEAD)
    split = qkv_rows.reshape(num_seqs, seq_len, 3, heads, HEAD)
    scores = mm('bqhc,bkhc->bhqk', split[:, :, 0], split[:, :, 1]) * (HEAD ** -0.5)
    rows = lax.broadcasted_iota(jnp.int32, (seq_len, seq_len), 0)
    cols = lax.broadcasted_iota(jnp.int32, (seq_len, seq_len), 1)
    scores = jnp.where(rows >= cols, scores, -1e30)
    prob_rows = jax.nn.softmax(scores, axis=-1).astype(BF16)
    mixed = mm('bhqk,bkhc->bqhc', prob_rows, split[:, :, 2])
    return mixed.astype(BF16).reshape(num_seqs, seq_len, heads * HEAD)


def slot_codes(idx_rows, experts, cap):
    tokens = idx_rows.shape[0]
    chosen = jnp.any(idx_rows[:, :, None] == jnp.arange(experts, dtype=jnp.int32), axis=1).astype(BF16)
    rows = lax.broadcasted_iota(jnp.int32, (tokens, tokens), 0)
    cols = lax.broadcasted_iota(jnp.int32, (tokens, tokens), 1)
    prior = mm('se,st->et', chosen, (rows < cols).astype(BF16))
    taken = mm('se,st->et', chosen, (rows == cols).astype(BF16))
    return jnp.where(taken > 0.5, jnp.where(prior < cap, prior, DROPPED), UNCHOSEN).astype(BF16)


def one_hot(codes, cap):
    slots = lax.broadcasted_iota(jnp.int32, codes.shape[:-1] + (cap, codes.shape[-1]), codes.ndim - 1)
    return (codes[..., None, :].astype(F32) == slots.astype(F32)).astype(BF16)


def gates_of(xn, codes, w_router):
    logits = mm('...td,de->...et', xn, w_router)
    prob = jax.nn.softmax(logits, axis=-2)
    mask = (codes.astype(F32) < UNCHOSEN - 1.0).astype(F32)
    picked = prob * mask
    total = jnp.sum(picked, axis=-2, keepdims=True)
    return prob, mask, picked / total, total


def after(value, *deps):
    return lax.optimization_barrier((value,) + deps)[0]


HALF = 768
CHUNK = 64
STEPS = HALF // CHUNK
BLOCK = 128
MESH = pl.DeviceIdType.MESH


def dot_tn(a, b):
    return lax.dot_general(a, b, (((0,), (0,)), ((), ())), preferred_element_type=jnp.float32)


def dense_kernel(acts_xn_ref, acts_ao_ref, dsend_ref, gains_ref, router_ref, low_ref, high_ref, gains_out_ref, router_out_ref,
                 dall, part, z_in, total, gain_buf, router_buf,
                 d_send, d_recv, dp_send, dp_recv, z_send, z_recv, own_sem, g_send, g_recv, r_send, r_recv, s_send, s_recv):
    z = lax.axis_index('dp')
    ep = lax.axis_index('ep')
    core = lax.rem(ep, 2)
    quarter = ep // 2
    width = dsend_ref.shape[2]
    split = width * 3 // 4
    tokens = dsend_ref.shape[1]
    partner = ep + 1 - 2 * core
    bit_x = lax.rem(quarter, 2)
    bit_y = quarter // 2
    flip = lambda bx, by: 2 * ((bit_x + bx - 2 * bit_x * bx) + 2 * (bit_y + by - 2 * bit_y * by)) + core
    x_dev, y_dev, xy_dev = flip(1, 0), flip(0, 1), flip(1, 1)
    inner = jnp.logical_or(z == 1, z == 2)
    z_mate = jnp.where(z == 0, 1, jnp.where(z == 1, 0, jnp.where(z == 2, 3, 2)))
    z_cross = 3 - z

    def copy(src, dst, s_sem, r_sem, dp, e):
        return pltpu.make_async_remote_copy(src_ref=src, dst_ref=dst, send_sem=s_sem, recv_sem=r_sem,
                                            device_id=(dp, e), device_id_type=MESH)

    rows_of = lambda e: pl.ds(pl.multiple_of(e * tokens, tokens), tokens)
    far = (x_dev, y_dev, xy_dev)
    for i, dev in enumerate(far):
        copy(dsend_ref.at[dev // 2], dall.at[rows_of(ep)], d_send.at[i], d_recv.at[i], z, dev).start()
    copy(dsend_ref.at[quarter], dall.at[rows_of(ep)], dp_send.at[3], dp_recv.at[3], z, partner).start()

    world = router_ref.shape[0]
    me = z * 8 + ep

    def push(pick, buf, s_sem, r_sem, d, target):
        return copy(pick(target), buf.at[me], s_sem.at[d], r_sem.at[d], target // 8, lax.rem(target, 8))

    def push_all(*args):
        def body(d, _):
            push(*args, d, lax.rem(me + d, world)).start()
            return 0

        lax.fori_loop(1, world, body, 0)

    def wait_all(pick, buf, s_sem, r_sem):
        def body(d, _):
            push(pick, buf, s_sem, r_sem, d, lax.rem(me + d, world)).wait()
            return 0

        lax.fori_loop(1, world, body, 0)

    def device_sum(buf):
        return lax.fori_loop(0, world, lambda s, acc: acc + buf[s], jnp.zeros(buf.shape[1:], jnp.float32))

    gain_push = (lambda t: gains_ref, gain_buf, g_send, g_recv)
    share_push = (lambda t: router_ref.at[t], router_buf, r_send, r_recv)
    total_push = (lambda t: router_out_ref.at[me], router_out_ref, s_send, s_recv)
    push_all(*gain_push)
    push_all(*share_push)

    dall[rows_of(ep), :] = dsend_ref[quarter]
    for i, dev in enumerate(far):
        copy(dsend_ref.at[dev // 2], dall.at[rows_of(dev)], d_send.at[i], d_recv.at[i], z, dev).wait_recv()
        copy(dall.at[rows_of(dev)], dall.at[rows_of(dev)], dp_send.at[i], dp_recv.at[i], z, partner).start()
    for i, dev in enumerate(far + (ep,)):
        other = dev + 1 - 2 * core
        copy(dsend_ref.at[0], dall.at[rows_of(other)], dp_send.at[i], dp_recv.at[i], z, partner).wait_recv()

    up_copy = lambda k: copy(part.at[k], z_in.at[k], z_send.at[0, k], z_recv.at[0, k], z_mate, ep)
    cross_copy = lambda k: copy(part.at[k], total.at[k], z_send.at[1, k], z_recv.at[1, k], z_cross, ep)
    down_copy = lambda k: copy(total.at[k], total.at[k], z_send.at[2, k], z_recv.at[2, k], z_mate, ep)

    def own_copy(k):
        ref = low_ref if k < STEPS // 2 else high_ref
        return pltpu.make_async_copy(total.at[k], ref.at[pl.ds(k % (STEPS // 2) * CHUNK, CHUNK), :], own_sem.at[k])

    for i in range(STEPS + 3):
        k = i
        if k < STEPS and k * CHUNK % BLOCK == 0:
            cols = slice(k * CHUNK, k * CHUNK + BLOCK)
            many = BLOCK // CHUNK
            part[k:k + many, :, :split] = dot_tn(acts_xn_ref[:, cols], dall[:, :split]).reshape(many, CHUNK, split)
            part[k:k + many, :, split:] = dot_tn(acts_ao_ref[:, cols], dall[:, split:]).reshape(many, CHUNK, width - split)
        if i == 6:
            wait_all(*share_push)
            router_buf[me] = router_ref[me]
            router_out_ref[me] = device_sum(router_buf)
        if i == 8:
            push_all(*total_push)
        a = i - 1
        t = i - 2

        @pl.when(inner)
        def _():
            if 0 <= a < STEPS:
                up_copy(a).wait_recv()
                part[a] = part[a] + z_in[a]
                cross_copy(a).start()
            if 0 <= t < STEPS:
                cross_copy(t).wait_recv()
                total[t] = part[t] + total[t]
                down_copy(t).start()
                own_copy(t).start()

        @pl.when(jnp.logical_not(inner))
        def _():
            if k < STEPS:
                up_copy(k).start()
            if 0 <= i - 3 < STEPS:
                down_copy(i - 3).wait_recv()
                own_copy(i - 3).start()

    for k in range(STEPS):
        own_copy(k).wait()

    @pl.when(inner)
    def _():
        for k in range(STEPS):
            cross_copy(k).wait_send()
            down_copy(k).wait_send()

    @pl.when(jnp.logical_not(inner))
    def _():
        for k in range(STEPS):
            up_copy(k).wait_send()

    for i, dev in enumerate(far):
        copy(dsend_ref.at[dev // 2], dall.at[rows_of(ep)], d_send.at[i], d_recv.at[i], z, dev).wait_send()
        copy(dall.at[rows_of(dev)], dall.at[rows_of(dev)], dp_send.at[i], dp_recv.at[i], z, partner).wait_send()
    copy(dsend_ref.at[quarter], dall.at[rows_of(ep)], dp_send.at[3], dp_recv.at[3], z, partner).wait_send()

    wait_all(*gain_push)
    gain_buf[me] = gains_ref[...]
    gains_out_ref[...] = device_sum(gain_buf)
    wait_all(*total_push)


def dense_sums(acts_xn, acts_ao, dsend, gains, router):
    rows, width = acts_xn.shape[0], dsend.shape[2]
    any_spec = pl.BlockSpec(memory_space=pl.ANY)
    vmem = pl.BlockSpec(memory_space=pltpu.VMEM)
    dma = pltpu.SemaphoreType.DMA
    f32 = lambda *shape: jax.ShapeDtypeStruct(shape, jnp.float32)
    world = router.shape[0]
    return pl.pallas_call(
        dense_kernel,
        out_shape=(f32(HALF // 2, width), f32(HALF // 2, width), f32(*gains.shape), f32(*router.shape)),
        in_specs=[vmem, vmem, vmem, vmem, vmem],
        out_specs=(any_spec, any_spec, vmem, vmem),
        scratch_shapes=[
            pltpu.VMEM((rows, width), jnp.bfloat16),
            pltpu.VMEM((STEPS, CHUNK, width), jnp.float32),
            pltpu.VMEM((STEPS, CHUNK, width), jnp.float32),
            pltpu.VMEM((STEPS, CHUNK, width), jnp.float32),
            pltpu.VMEM((world,) + gains.shape, jnp.float32),
            pltpu.VMEM(router.shape, jnp.float32),
            dma((3,)), dma((3,)), dma((4,)), dma((4,)), dma((3, STEPS)), dma((3, STEPS)), dma((STEPS,)),
            dma((world,)), dma((world,)), dma((world,)), dma((world,)), dma((world,)), dma((world,)),
        ],
        compiler_params=pltpu.CompilerParams(has_side_effects=True, vmem_limit_bytes=48 << 20),
        cost_estimate=pl.CostEstimate(flops=100 * 10**9, bytes_accessed=40 << 20, transcendentals=0),
        name='dense_sums',
    )(acts_xn, acts_ao, dsend, gains, router)


def assemble_kernel(*refs):
    pieces, (qkv_ref, wo_ref, buf, in_sem, out_sem) = refs[:16], refs[16:]
    ep = lax.axis_index('ep')
    bits = (lax.rem(ep, 2), lax.rem(ep // 2, 2), ep // 4)
    size = HALF // 2
    width = buf.shape[2]
    split = width * 3 // 4

    def load(n):
        return pltpu.make_async_copy(pieces[n], buf.at[n % 4], in_sem.at[n % 4])

    def stores(n):
        flips = (n // 2 % 2, n // 4 % 2, n // 8)
        core, bx, by = [b + f - 2 * b * f for b, f in zip(bits, flips)]
        rows = pl.ds(pl.multiple_of(core * HALF + n % 2 * size, size), size)
        q = bx + 2 * by
        return [pltpu.make_async_copy(buf.at[n % 4, :, pl.ds(lo, cols)],
                                      ref.at[rows, pl.ds(pl.multiple_of(q * cols, 128), cols)], out_sem.at[n % 4, i])
                for i, (ref, lo, cols) in enumerate(((qkv_ref, 0, split), (wo_ref, split, width - split)))]

    for n in range(16 + 2):
        if n < 16:
            if n >= 4:
                for c in stores(n - 4):
                    c.wait()
            load(n).start()
        if n >= 2:
            load(n - 2).wait()
            for c in stores(n - 2):
                c.start()
    for n in range(12, 16):
        for c in stores(n):
            c.wait()


def assemble(pieces):
    width = pieces[0].shape[1]
    any_spec = pl.BlockSpec(memory_space=pl.ANY)
    return pl.pallas_call(
        assemble_kernel,
        out_shape=(jax.ShapeDtypeStruct((2 * HALF, 3 * width), F32), jax.ShapeDtypeStruct((2 * HALF, width), F32)),
        in_specs=[any_spec] * 16,
        out_specs=(any_spec, any_spec),
        scratch_shapes=[pltpu.VMEM((4, HALF // 2, width), F32), pltpu.SemaphoreType.DMA((4,)), pltpu.SemaphoreType.DMA((4, 2))],
        compiler_params=pltpu.CompilerParams(vmem_limit_bytes=24 << 20),
        cost_estimate=pl.CostEstimate(flops=20 * 10**9, bytes_accessed=80 << 20, transcendentals=0),
        name='assemble',
    )(*pieces)


def dot_nn(a, b):
    return lax.dot_general(a, b, (((1,), (0,)), ((), ())), preferred_element_type=jnp.float32)


def dot_nt(a, b):
    return lax.dot_general(a, b, (((1,), (1,)), ((), ())), preferred_element_type=jnp.float32)


def slot_select(codes_t, gates, first, local_exp, cap, codes_buf, gates_buf):
    tokens = codes_t.shape[1]
    codes_buf[...] = codes_t
    gates_buf[...] = gates
    my_codes = codes_buf[pl.ds(first, local_exp), :]
    my_gates = gates_buf[pl.ds(first, local_exp), :]
    slots = lax.broadcasted_iota(jnp.int32, (local_exp, cap, tokens), 1).astype(F32)
    select = jnp.where(my_codes[:, None, :] == slots, 1.0, 0.0)
    gate_slot = jnp.sum(select * my_gates[:, None, :], axis=-1, keepdims=True).reshape(local_exp * cap, 1)
    return select.reshape(local_exp * cap, tokens).astype(BF16), gate_slot


def slot_rows(xn, dyc, router, first, local_exp, cap, codes_buf, gates_buf):
    experts = router.shape[0]
    width = xn.shape[1]
    codes = dyc[:, width:].astype(F32).T[:experts]
    logits = dot_nt(router, xn)
    prob = jnp.exp(logits - jnp.max(logits, axis=0, keepdims=True))
    prob = prob / jnp.sum(prob, axis=0, keepdims=True)
    picked = jnp.where(codes < UNCHOSEN - 1.0, prob, 0.0)
    gates = picked / jnp.sum(picked, axis=0, keepdims=True)
    select, gate_slot = slot_select(codes, gates, first, local_exp, cap, codes_buf, gates_buf)
    return dot_nn(select, xn).astype(BF16), dot_nn(select, dyc[:, :width]), gate_slot


def dispatch_kernel(local_exp, cap, rows_ref, router_ref, recv_in, d_recv_in, recv_ref, d_recv_ref, codes_buf, gates_buf):
    first = pl.multiple_of(lax.axis_index('ep') * local_exp, local_exp)
    router = router_ref[...]
    width = router.shape[1]
    for i in range(rows_ref.shape[0]):
        recv, dy_rows, gate_slot = slot_rows(rows_ref[i, :, :width], rows_ref[i, :, width:], router, first, local_exp, cap,
                                             codes_buf.at[i], gates_buf.at[i])
        at = slice(i * cap, (i + 1) * cap)
        recv_ref[:, at, :] = recv.reshape(local_exp, cap, width)
        d_recv_ref[:, at, :] = (gate_slot * dy_rows).astype(BF16).reshape(local_exp, cap, width)


def dispatch_rows(rows, router_t, recv, d_recv, skip, cap):
    sources, tokens, lanes = rows.shape
    local_exp, _, width = recv.shape
    experts = router_t.shape[0]
    step = 4
    any_spec = pl.BlockSpec(memory_space=pl.ANY)
    out_spec = pl.BlockSpec((local_exp, step * cap, width), lambda s: (0, skip // (step * cap) + s, 0))
    same = lambda arr: jax.ShapeDtypeStruct(arr.shape, arr.dtype)
    return pl.pallas_call(
        functools.partial(dispatch_kernel, local_exp, cap),
        grid=(sources // step,),
        in_specs=[pl.BlockSpec((step, tokens, lanes), lambda s: (s, 0, 0)), pl.BlockSpec(router_t.shape, lambda s: (0, 0)), any_spec, any_spec],
        out_specs=(out_spec, out_spec),
        scratch_shapes=[pltpu.VMEM((step, experts, tokens), F32), pltpu.VMEM((step, experts, tokens), F32)],
        out_shape=(same(recv), same(d_recv)),
        input_output_aliases={2: 0, 3: 1},
        compiler_params=pltpu.CompilerParams(vmem_limit_bytes=56 << 20),
        cost_estimate=pl.CostEstimate(flops=sources * 4 * local_exp * cap * tokens * width, transcendentals=0,
                                      bytes_accessed=sources * tokens * width * 8),
        name='dispatch_rows',
    )(rows, router_t, recv, d_recv)


def hidden_grads(recv, d_recv, up, lin, down):
    u = dot_nn(recv, up).astype(BF16).astype(F32)
    v = dot_nn(recv, lin).astype(BF16).astype(F32)
    d_act = dot_nt(d_recv, down).astype(BF16).astype(F32)
    sig = jax.nn.sigmoid(u)
    act = u * sig
    d_u = d_act * v * (sig + act * (1.0 - sig))
    return (act * v).astype(BF16), d_u.astype(BF16), (d_act * act).astype(BF16)


def moe_kernel(cap, xn_ref, dyc_ref, router_ref, up_ref, lin_ref, down_ref, back_ref, gate_back_ref, recv_out, d_recv_out,
               xn_all, recv, d_recv, dy_rows, d_tok, gate_send, up_buf, lin_buf, down_buf, codes_buf, gates_buf,
               w_sem, x_send, x_recv, p_send, p_recv, own_sem, row_sem, b_send, b_recv, g_send, g_recv):
    z = lax.axis_index('dp')
    ep = lax.axis_index('ep')
    local_exp = up_ref.shape[0]
    plane = xn_all.shape[0]
    width = xn_ref.shape[1]
    first = pl.multiple_of(ep * local_exp, local_exp)
    bits = (lax.rem(ep, 2), lax.rem(ep // 2, 2), ep // 4)

    def flipped(d):
        flags = (lax.rem(d, 2), lax.rem(d // 2, 2), d // 4)
        both = [b + f - 2 * b * f for b, f in zip(bits, flags)]
        return both[0] + 2 * both[1] + 4 * both[2]

    def copy(src, dst, s_sem, r_sem, dev):
        return pltpu.make_async_remote_copy(src_ref=src, dst_ref=dst, send_sem=s_sem, recv_sem=r_sem,
                                            device_id=(z, dev), device_id_type=MESH)

    def weights(e, slot):
        return [pltpu.make_async_copy(src.at[e], dst.at[slot], w_sem.at[i, slot])
                for i, (src, dst) in enumerate(((up_ref, up_buf), (lin_ref, lin_buf), (down_ref, down_buf)))]

    for i in (1, 2, 3):
        copy(xn_ref, xn_all.at[ep], x_send.at[i], x_recv.at[i], flipped(2 * i)).start()
    copy(xn_ref, xn_all.at[ep], p_send.at[0], p_recv.at[0], flipped(1)).start()
    for c in weights(0, 0):
        c.start()
    xn_all[ep] = xn_ref[...]
    router = router_ref[...]

    def pair(i, _):
        near = flipped(2 * i)
        other = flipped(2 * i + 1)

        @pl.when(i > 0)
        def _():
            copy(xn_ref, xn_all.at[near], x_send.at[i], x_recv.at[i], near).wait_recv()
            copy(xn_all.at[near], xn_all.at[near], p_send.at[i], p_recv.at[i], flipped(1)).start()

        copy(xn_ref, xn_all.at[other], p_send.at[i], p_recv.at[i], flipped(1)).wait_recv()
        for j, src in enumerate((near, other)):
            rows, dy, gate_slot = slot_rows(xn_all[src], dyc_ref[src], router, first, local_exp, cap, codes_buf.at[j], gates_buf.at[j])
            at = pl.ds(pl.multiple_of(src * cap, cap), cap)
            recv[:, at, :] = rows.reshape(local_exp, cap, width)
            dy_rows[:, at, :] = dy.astype(BF16).reshape(local_exp, cap, width)
            d_recv[:, at, :] = (gate_slot * dy).astype(BF16).reshape(local_exp, cap, width)
        return 0

    lax.fori_loop(0, plane // 2, pair, 0)

    keep = [pltpu.make_async_copy(src, dst.at[:, pl.ds(0, plane * cap), :], row_sem.at[i])
            for i, (src, dst) in enumerate(((recv, recv_out), (d_recv, d_recv_out)))]
    for c in keep:
        c.start()

    def home(d, e):
        dev = flipped(d)
        src = d_tok.at[e, pl.ds(pl.multiple_of(dev * cap, cap), cap), :]
        return copy(src, back_ref.at[first + e], b_send.at[d, e], b_recv.at[d, e], dev)

    def stay(e):
        return pltpu.make_async_copy(d_tok.at[e, pl.ds(pl.multiple_of(ep * cap, cap), cap), :], back_ref.at[first + e], own_sem.at[e])

    def expert(e, _):
        slot = lax.rem(e, 2)

        @pl.when(e + 1 < local_exp)
        def _():
            for c in weights(e + 1, 1 - slot):
                c.start()

        for c in weights(e, slot):
            c.wait()
        up, lin, down = up_buf[slot], lin_buf[slot], down_buf[slot]
        act, d_u, d_v = hidden_grads(recv[e], d_recv[e], up, lin, down)
        d_tok[e] = (dot_nt(d_u, up) + dot_nt(d_v, lin)).astype(BF16)
        y = dot_nn(act, down).astype(BF16).astype(F32)
        d_gate = jnp.sum(dy_rows[e].astype(F32) * y, axis=-1, keepdims=True)
        lane = lax.broadcasted_iota(jnp.int32, (plane, cap, 128), 2)
        row = lax.broadcasted_iota(jnp.int32, (plane, cap, 128), 1)
        wide = jnp.broadcast_to(d_gate, (plane * cap, 128)).reshape(plane, cap, 128)
        gate_send[:, pl.ds(e, 1), :] = jnp.sum(jnp.where(lane == row, wide, 0.0), axis=1, keepdims=True)
        for d in (6, 7, 2, 3, 4, 5, 1):
            home(d, e).start()
        stay(e).start()
        return 0

    lax.fori_loop(0, local_exp, expert, 0)

    for c in keep:
        c.wait()

    def gate_home(d):
        dev = flipped(d)
        return copy(gate_send.at[dev], gate_back_ref.at[ep], g_send.at[d], g_recv.at[d], dev)

    for d in range(1, plane):
        gate_home(d).start()
    gate_back_ref[ep] = gate_send[ep]

    def drain(e, _):
        for d in range(1, plane):
            src = d_tok.at[0, pl.ds(0, cap), :]
            copy(src, back_ref.at[flipped(d) * local_exp + e], b_send.at[d, e], b_recv.at[d, e], flipped(d)).wait_recv()
            home(d, e).wait_send()
        stay(e).wait()
        return 0

    lax.fori_loop(0, local_exp, drain, 0)
    for d in range(1, plane):
        copy(gate_send.at[0], gate_back_ref.at[flipped(d)], g_send.at[d], g_recv.at[d], flipped(d)).wait_recv()
        gate_home(d).wait_send()
    for i in (1, 2, 3):
        copy(xn_ref, xn_all.at[ep], x_send.at[i], x_recv.at[i], flipped(2 * i)).wait_send()
        copy(xn_all.at[flipped(2 * i)], xn_all.at[flipped(2 * i)], p_send.at[i], p_recv.at[i], flipped(1)).wait_send()
    copy(xn_ref, xn_all.at[ep], p_send.at[0], p_recv.at[0], flipped(1)).wait_send()


def moe_backward(xn, dyc_plane, router_t, w_up, w_lin, w_down, cap, planes):
    plane, tokens = dyc_plane.shape[:2]
    local_exp, width, hid = w_up.shape
    experts = router_t.shape[0]
    rows = pltpu.VMEM((local_exp, plane * cap, width), BF16)
    vmem = pl.BlockSpec(memory_space=pltpu.VMEM)
    any_spec = pl.BlockSpec(memory_space=pl.ANY)
    dma = pltpu.SemaphoreType.DMA
    return pl.pallas_call(
        functools.partial(moe_kernel, cap),
        out_shape=(jax.ShapeDtypeStruct((experts, cap, width), BF16), jax.ShapeDtypeStruct((plane, local_exp, 128), F32),
                   jax.ShapeDtypeStruct((local_exp, planes * plane * cap, width), BF16),
                   jax.ShapeDtypeStruct((local_exp, planes * plane * cap, width), BF16)),
        in_specs=[vmem, vmem, vmem, any_spec, any_spec, any_spec],
        out_specs=(any_spec, vmem, any_spec, any_spec),
        scratch_shapes=[
            pltpu.VMEM((plane, tokens, width), BF16), rows, rows, rows, rows, pltpu.VMEM((plane, local_exp, 128), F32),
            pltpu.VMEM((2, width, hid), BF16), pltpu.VMEM((2, width, hid), BF16), pltpu.VMEM((2, hid, width), BF16),
            pltpu.VMEM((2, experts, tokens), F32), pltpu.VMEM((2, experts, tokens), F32),
            dma((3, 2)), dma((4,)), dma((4,)), dma((4,)), dma((4,)), dma((local_exp,)), dma((2,)),
            dma((plane, local_exp)), dma((plane, local_exp)), dma((plane,)), dma((plane,)),
        ],
        compiler_params=pltpu.CompilerParams(has_side_effects=True, vmem_limit_bytes=60 << 20),
        cost_estimate=pl.CostEstimate(flops=60 * 10**9, bytes_accessed=64 << 20, transcendentals=0),
        name='moe_backward',
    )(xn, dyc_plane, router_t, w_up, w_lin, w_down)


def weight_kernel(recv_ref, d_recv_ref, up_ref, lin_ref, down_ref, *rest):
    g_up_ref, g_lin_ref, g_down_ref, act_buf, du_buf, dv_buf = rest[-6:]
    total = recv_ref.shape[1]
    block = 256

    @pl.loop(0, total // block)
    def _(i):
        rows = pl.ds(pl.multiple_of(i * block, block), block)
        act, d_u, d_v = hidden_grads(recv_ref[0, rows, :], d_recv_ref[0, rows, :], up_ref[0], lin_ref[0], down_ref[0])
        act_buf[rows, :] = act
        du_buf[rows, :] = d_u
        dv_buf[rows, :] = d_v

    width = recv_ref.shape[2]
    cols = 512

    @pl.loop(0, width // cols)
    def _(i):
        c = pl.ds(pl.multiple_of(i * cols, cols), cols)
        g_up_ref[0, c, :] = dot_tn(recv_ref[0, :, c], du_buf[...])
        g_lin_ref[0, c, :] = dot_tn(recv_ref[0, :, c], dv_buf[...])
        g_down_ref[0, :, c] = dot_tn(act_buf[...], d_recv_ref[0, :, c])


def weight_grads(recv, d_recv, w_up, w_lin, w_down, first, count, grads=()):
    _, total, width = recv.shape
    hid = w_up.shape[2]
    rows = pl.BlockSpec((1, total, width), lambda e: (first + e, 0, 0))
    wide = pl.BlockSpec((1, width, hid), lambda e: (first + e, 0, 0))
    tall = pl.BlockSpec((1, hid, width), lambda e: (first + e, 0, 0))
    f32 = lambda arr: jax.ShapeDtypeStruct(arr.shape, F32)
    return pl.pallas_call(
        weight_kernel,
        grid=(count,),
        out_shape=(f32(w_up), f32(w_lin), f32(w_down)),
        in_specs=[rows, rows, wide, wide, tall] + [pl.BlockSpec(memory_space=pl.ANY)] * len(grads),
        out_specs=(wide, wide, tall),
        scratch_shapes=[pltpu.VMEM((total, hid), BF16)] * 3,
        input_output_aliases={5 + i: i for i in range(len(grads))},
        compiler_params=pltpu.CompilerParams(vmem_limit_bytes=60 << 20),
        cost_estimate=pl.CostEstimate(flops=12 * count * total * width * hid, transcendentals=0, bytes_accessed=count * (20 << 20)),
        name='weight_grads',
    )(recv, d_recv, w_up, w_lin, w_down, *grads)


def solution(mesh):
    tok_spec = P(('dp', 'ep'))
    exp_spec = P('ep')
    rep_spec = P()

    def local(x_in, dy_in, route_idx, gain_attn, w_qkv, w_o, gain_ffn, w_router, w_up, w_lin, w_down):
        num_seqs, seq_len, width = x_in.shape
        tokens = num_seqs * seq_len
        top = route_idx.shape[-1]
        experts = w_router.shape[1]
        local_exp = w_up.shape[0]
        cap = ((tokens * top * 5) // (experts * 4) + 7) // 8 * 8
        ep_size = mesh.shape['ep']

        codes = slot_codes(route_idx.reshape(tokens, top), experts, cap)
        dy_own = dy_in.reshape(tokens, width)
        lanes = jnp.zeros((tokens, HEAD - experts), BF16)
        dyc_own = jnp.concatenate([dy_own, codes.T, lanes], axis=1)
        dyc_plane = lax.all_gather(dyc_own, 'ep')
        router_t = w_router.T
        planes = mesh.shape['dp']

        def spread(act):
            halves = jnp.moveaxis(act.reshape(tokens, 2, width // 2), 1, 0)
            send = jnp.broadcast_to(halves[None], (ep_size // 2, 2, tokens, width // 2)).reshape(ep_size, tokens, width // 2)
            return lax.all_to_all(send, 'ep', 0, 0).reshape(ep_size * tokens, width // 2)

        x_f = x_in.astype(F32)
        xn_one, norm_one_pull = jax.vjp(rms_norm, x_f, gain_attn.astype(F32))
        acts_xn = spread(xn_one)
        qkv_all = mm('bsd,de->bse', xn_one, w_qkv).astype(BF16)
        attn_out, attn_pull = jax.vjp(attn_core, qkv_all)
        attn_proj = mm('bsd,de->bse', attn_out, w_o)
        hidden = (x_f + attn_proj).astype(BF16).astype(F32).reshape(tokens, width)
        xn_two, norm_two_pull = jax.vjp(rms_norm, hidden, gain_ffn.astype(F32))

        rows_own = jnp.concatenate([xn_two, dyc_own], axis=1)
        foreign = [lax.ppermute(rows_own, 'dp', [((z + r) % planes, z) for z in range(planes)]) for r in range(1, planes)]
        d_back, gate_back, recv, d_recv = moe_backward(xn_two, dyc_plane, router_t, w_up, w_lin, w_down, cap, planes)
        acts_ao = spread(after(attn_out, gate_back))
        d_gate_back = gate_back[:, :, :cap].reshape(experts, cap)

        select_own = one_hot(codes, cap)
        d_moe_in = mm('ect,ecd->td', select_own, d_back)
        prob, mask, gates, total = gates_of(xn_two, codes, w_router)
        d_gates = jnp.sum(select_own.astype(F32) * d_gate_back[:, :, None], axis=1)
        d_picked = (d_gates - jnp.sum(d_gates * gates, axis=0, keepdims=True)) / total * mask
        d_logits = (prob * (d_picked - jnp.sum(prob * d_picked, axis=0, keepdims=True))).astype(BF16)
        d_xn_two = (d_moe_in + mm('et,de->td', d_logits, w_router)).astype(BF16)
        grad_router = mm('td,et->de', xn_two, d_logits)
        d_hidden, grad_gain_ffn = norm_two_pull(d_xn_two)
        d_resid = (d_hidden + dy_own.astype(F32)).astype(BF16).reshape(num_seqs, seq_len, width)
        d_attn_out = mm('bse,de->bsd', d_resid, w_o).astype(BF16)
        d_qkv = attn_pull(d_attn_out)[0]
        foreign = lax.all_gather(jnp.stack(foreign), 'ep')
        d_xn_one = mm('bse,de->bsd', d_qkv, w_qkv).astype(BF16)
        d_x_norm, grad_gain_attn = norm_one_pull(d_xn_one)
        dx_out = (d_x_norm + d_resid.astype(F32)).astype(BF16)
        quarters = lambda arr: jnp.moveaxis(arr.reshape(tokens, 4, -1), 1, 0)
        dsend = jnp.concatenate([quarters(d_qkv), quarters(d_resid)], axis=2)
        gains = jnp.concatenate([grad_gain_attn, grad_gain_ffn]).reshape(-1, 128)
        world_size = planes * ep_size
        low, high, gains, grad_router = dense_sums(acts_xn, acts_ao, dsend, gains, grad_router.reshape(world_size, -1, 128))
        grad_router = grad_router.reshape(width, experts)
        grad_gain_attn, grad_gain_ffn = gains.reshape(2, width)

        flip = lambda arr, bit: lax.ppermute(arr, 'ep', [(e, e ^ bit) for e in range(ep_size)])
        low_x, high_y = flip(low, 2), flip(high, 4)
        low_y, high_x = flip(low, 4), flip(high, 2)
        low_xy, high_xy = flip(low_x, 4), flip(high_y, 2)
        pieces = [low, high, low_x, high_x, low_y, high_y, low_xy, high_xy]
        swapped = [flip(arr, 1) for arr in pieces[:6]]
        swapped += [flip(arr, 1) for arr in pieces[6:]]
        pieces = [arr for i in range(4) for arr in (pieces[2 * i], pieces[2 * i + 1], swapped[2 * i], swapped[2 * i + 1])]

        foreign = after(foreign, gains)
        recv, d_recv = dispatch_rows(foreign.reshape(-1, tokens, foreign.shape[-1]), router_t, recv, d_recv, ep_size * cap, cap)
        grads, first = (), 0
        for count in (local_exp // 4, local_exp // 4, local_exp // 2):
            grads = weight_grads(recv, d_recv, w_up, w_lin, w_down, first, count, grads)
            first += count
        grad_up, grad_lin, grad_down = grads
        grad_wqkv, grad_wo = assemble(pieces)
        return (dx_out, grad_gain_attn, grad_wqkv, grad_wo, grad_gain_ffn, grad_router, grad_up, grad_lin, grad_down)

    in_specs = (tok_spec, tok_spec, tok_spec, rep_spec, rep_spec, rep_spec, rep_spec, rep_spec, exp_spec, exp_spec, exp_spec)
    out_specs = (tok_spec, rep_spec, rep_spec, rep_spec, rep_spec, rep_spec, exp_spec, exp_spec, exp_spec)

    return jax.shard_map(local, mesh=mesh, in_specs=in_specs, out_specs=out_specs, check_vma=False)
```

```python
import functools

import jax
import jax.numpy as jnp
from jax import lax
from jax.experimental import pallas as pl
from jax.experimental.pallas import tpu as pltpu
from jax.sharding import PartitionSpec as P


EPS = 1e-6
HEAD = 128
DROPPED = 64.0
UNCHOSEN = 128.0
F32 = jnp.float32
BF16 = jnp.bfloat16


def mm(spec, a, b):
    return jnp.einsum(spec, a, b, preferred_element_type=F32)


def rms_norm(values, gain):
    scale = lax.rsqrt(jnp.mean(values * values, axis=-1, keepdims=True) + EPS)
    return (values * scale * gain).astype(BF16)


def attn_core(qkv_rows):
    num_seqs, seq_len, width = qkv_rows.shape
    heads = width // (3 * HEAD)
    split = qkv_rows.reshape(num_seqs, seq_len, 3, heads, HEAD)
    scores = mm('bqhc,bkhc->bhqk', split[:, :, 0], split[:, :, 1]) * (HEAD ** -0.5)
    rows = lax.broadcasted_iota(jnp.int32, (seq_len, seq_len), 0)
    cols = lax.broadcasted_iota(jnp.int32, (seq_len, seq_len), 1)
    scores = jnp.where(rows >= cols, scores, -1e30)
    prob_rows = jax.nn.softmax(scores, axis=-1).astype(BF16)
    mixed = mm('bhqk,bkhc->bqhc', prob_rows, split[:, :, 2])
    return mixed.astype(BF16).reshape(num_seqs, seq_len, heads * HEAD)


def slot_codes(idx_rows, experts, cap):
    tokens = idx_rows.shape[0]
    chosen = jnp.any(idx_rows[:, :, None] == jnp.arange(experts, dtype=jnp.int32), axis=1).astype(BF16)
    rows = lax.broadcasted_iota(jnp.int32, (tokens, tokens), 0)
    cols = lax.broadcasted_iota(jnp.int32, (tokens, tokens), 1)
    prior = mm('se,st->et', chosen, (rows < cols).astype(BF16))
    taken = mm('se,st->et', chosen, (rows == cols).astype(BF16))
    return jnp.where(taken > 0.5, jnp.where(prior < cap, prior, DROPPED), UNCHOSEN).astype(BF16)


def one_hot(codes, cap):
    slots = lax.broadcasted_iota(jnp.int32, codes.shape[:-1] + (cap, codes.shape[-1]), codes.ndim - 1)
    return (codes[..., None, :].astype(F32) == slots.astype(F32)).astype(BF16)


def gates_of(xn, codes, w_router):
    logits = mm('...td,de->...et', xn, w_router)
    prob = jax.nn.softmax(logits, axis=-2)
    mask = (codes.astype(F32) < UNCHOSEN - 1.0).astype(F32)
    picked = prob * mask
    total = jnp.sum(picked, axis=-2, keepdims=True)
    return prob, mask, picked / total, total


def after(value, *deps):
    return lax.optimization_barrier((value,) + deps)[0]


HALF = 768
CHUNK = 64
STEPS = HALF // CHUNK
BLOCK = 128
MESH = pl.DeviceIdType.MESH


def dot_tn(a, b):
    return lax.dot_general(a, b, (((0,), (0,)), ((), ())), preferred_element_type=jnp.float32)


def dense_kernel(acts_xn_ref, acts_ao_ref, dsend_ref, gains_ref, router_ref, low_ref, high_ref, gains_out_ref, router_out_ref,
                 dall, stage, part, z_in, total, gain_buf, router_buf,
                 d_send, d_recv, h_send, h_recv, o_send, o_recv, dp_send, dp_recv, z_send, z_recv, own_sem,
                 g_send, g_recv, r_send, r_recv, s_send, s_recv):
    z = lax.axis_index('dp')
    ep = lax.axis_index('ep')
    core = lax.rem(ep, 2)
    quarter = ep // 2
    width = dsend_ref.shape[2]
    split = width * 3 // 4
    tokens = dsend_ref.shape[1]
    partner = ep + 1 - 2 * core
    bit_x = lax.rem(quarter, 2)
    bit_y = quarter // 2
    flip = lambda bx, by: 2 * ((bit_x + bx - 2 * bit_x * bx) + 2 * (bit_y + by - 2 * bit_y * by)) + core
    x_dev, y_dev, xy_dev = flip(1, 0), flip(0, 1), flip(1, 1)
    inner = jnp.logical_or(z == 1, z == 2)
    z_mate = jnp.where(z == 0, 1, jnp.where(z == 1, 0, jnp.where(z == 2, 3, 2)))
    z_cross = 3 - z

    def copy(src, dst, s_sem, r_sem, dp, e):
        return pltpu.make_async_remote_copy(src_ref=src, dst_ref=dst, send_sem=s_sem, recv_sem=r_sem,
                                            device_id=(dp, e), device_id_type=MESH)

    rows_of = lambda e: pl.ds(pl.multiple_of(e * tokens, tokens), tokens)
    far = (x_dev, y_dev, xy_dev)
    halves = pl.ds(0, tokens // 2), pl.ds(tokens // 2, tokens // 2)
    direct = lambda i: copy(dsend_ref.at[far[i] // 2], dall.at[rows_of(ep)], d_send.at[i], d_recv.at[i], z, far[i])
    hop = lambda n: copy(dsend_ref.at[xy_dev // 2, halves[n], :], stage.at[n], h_send.at[n], h_recv.at[n], z, far[n])

    def onward(n):
        at = pl.ds(pl.multiple_of(far[n] * tokens + n * (tokens // 2), tokens // 2), tokens // 2)
        return copy(stage.at[n], dall.at[at], o_send.at[n], o_recv.at[n], z, far[1 - n])

    def landed(n):
        at = pl.ds(pl.multiple_of(xy_dev * tokens + n * (tokens // 2), tokens // 2), tokens // 2)
        return copy(stage.at[n], dall.at[at], o_send.at[n], o_recv.at[n], z, far[1 - n])

    for n in range(2):
        hop(n).start()
    for i in range(2):
        direct(i).start()
    copy(dsend_ref.at[quarter], dall.at[rows_of(ep)], dp_send.at[3], dp_recv.at[3], z, partner).start()

    world = router_ref.shape[0]
    me = z * 8 + ep

    def push(pick, buf, s_sem, r_sem, d, target):
        return copy(pick(target), buf.at[me], s_sem.at[d], r_sem.at[d], target // 8, lax.rem(target, 8))

    def push_all(*args):
        def body(d, _):
            push(*args, d, lax.rem(me + d, world)).start()
            return _

        lax.fori_loop(1, world, body, 0)

    def wait_all(pick, buf, s_sem, r_sem):
        def body(d, _):
            push(pick, buf, s_sem, r_sem, d, lax.rem(me + d, world)).wait()
            return _

        lax.fori_loop(1, world, body, 0)

    def device_sum(buf):
        return lax.fori_loop(0, world, lambda s, acc: acc + buf[s], jnp.zeros(buf.shape[1:], jnp.float32))

    gain_push = (lambda t: gains_ref, gain_buf, g_send, g_recv)
    share_push = (lambda t: router_ref.at[t], router_buf, r_send, r_recv)
    total_push = (lambda t: router_out_ref.at[me], router_out_ref, s_send, s_recv)
    push_all(*gain_push)
    push_all(*share_push)

    dall[rows_of(ep), :] = dsend_ref[quarter]
    to_core = lambda i: copy(dall.at[rows_of(far[i])], dall.at[rows_of(far[i])], dp_send.at[i], dp_recv.at[i], z, partner)
    for n in range(2):
        hop(n).wait_recv()
        onward(n).start()
    for i in range(2):
        copy(dsend_ref.at[0], dall.at[rows_of(far[i])], d_send.at[i], d_recv.at[i], z, far[i]).wait_recv()
        to_core(i).start()
    for n in range(2):
        landed(n).wait_recv()
    to_core(2).start()
    for i, dev in enumerate(far + (ep,)):
        other = dev + 1 - 2 * core
        copy(dsend_ref.at[0], dall.at[rows_of(other)], dp_send.at[i], dp_recv.at[i], z, partner).wait_recv()

    up_copy = lambda k: copy(part.at[k], z_in.at[k], z_send.at[0, k], z_recv.at[0, k], z_mate, ep)
    cross_copy = lambda k: copy(part.at[k], total.at[k], z_send.at[1, k], z_recv.at[1, k], z_cross, ep)
    down_copy = lambda k: copy(total.at[k], total.at[k], z_send.at[2, k], z_recv.at[2, k], z_mate, ep)

    def own_copy(k):
        ref = low_ref if k < STEPS // 2 else high_ref
        return pltpu.make_async_copy(total.at[k], ref.at[pl.ds(k % (STEPS // 2) * CHUNK, CHUNK), :], own_sem.at[k])

    for i in range(STEPS + 3):
        k = i
        if k < STEPS and k * CHUNK % BLOCK == 0:
            cols = slice(k * CHUNK, k * CHUNK + BLOCK)
            many = BLOCK // CHUNK
            part[k:k + many, :, :split] = dot_tn(acts_xn_ref[:, cols], dall[:, :split]).reshape(many, CHUNK, split)
            part[k:k + many, :, split:] = dot_tn(acts_ao_ref[:, cols], dall[:, split:]).reshape(many, CHUNK, width - split)
        if i == 6:
            wait_all(*share_push)
            router_buf[me] = router_ref[me]
            router_out_ref[me] = device_sum(router_buf)
        if i == 8:
            push_all(*total_push)
        a = i - 1
        t = i - 2

        @pl.when(inner)
        def _():
            if 0 <= a < STEPS:
                up_copy(a).wait_recv()
                part[a] = part[a] + z_in[a]
                cross_copy(a).start()
            if 0 <= t < STEPS:
                cross_copy(t).wait_recv()
                total[t] = part[t] + total[t]
                down_copy(t).start()
                own_copy(t).start()

        @pl.when(jnp.logical_not(inner))
        def _():
            if k < STEPS:
                up_copy(k).start()
            if 0 <= i - 3 < STEPS:
                down_copy(i - 3).wait_recv()
                own_copy(i - 3).start()

    for k in range(STEPS):
        own_copy(k).wait()

    @pl.when(inner)
    def _():
        for k in range(STEPS):
            cross_copy(k).wait_send()
            down_copy(k).wait_send()

    @pl.when(jnp.logical_not(inner))
    def _():
        for k in range(STEPS):
            up_copy(k).wait_send()

    for n in range(2):
        direct(n).wait_send()
        hop(n).wait_send()
        onward(n).wait_send()
    for i in range(3):
        to_core(i).wait_send()
    copy(dsend_ref.at[quarter], dall.at[rows_of(ep)], dp_send.at[3], dp_recv.at[3], z, partner).wait_send()

    wait_all(*gain_push)
    gain_buf[me] = gains_ref[...]
    gains_out_ref[...] = device_sum(gain_buf)
    wait_all(*total_push)


def dense_sums(acts_xn, acts_ao, dsend, gains, router):
    rows, width = acts_xn.shape[0], dsend.shape[2]
    any_spec = pl.BlockSpec(memory_space=pl.ANY)
    vmem = pl.BlockSpec(memory_space=pltpu.VMEM)
    dma = pltpu.SemaphoreType.DMA
    f32 = lambda *shape: jax.ShapeDtypeStruct(shape, jnp.float32)
    world = router.shape[0]
    return pl.pallas_call(
        dense_kernel,
        out_shape=(f32(HALF // 2, width), f32(HALF // 2, width), f32(*gains.shape), f32(*router.shape)),
        in_specs=[vmem, vmem, vmem, vmem, vmem],
        out_specs=(any_spec, any_spec, vmem, vmem),
        scratch_shapes=[
            pltpu.VMEM((rows, width), jnp.bfloat16),
            pltpu.VMEM((2, dsend.shape[1] // 2, width), jnp.bfloat16),
            pltpu.VMEM((STEPS, CHUNK, width), jnp.float32),
            pltpu.VMEM((STEPS, CHUNK, width), jnp.float32),
            pltpu.VMEM((STEPS, CHUNK, width), jnp.float32),
            pltpu.VMEM((world,) + gains.shape, jnp.float32),
            pltpu.VMEM(router.shape, jnp.float32),
            *[dma((2,))] * 6, *[dma((4,))] * 2, dma((3, STEPS)), dma((3, STEPS)), dma((STEPS,)),
            dma((world,)), dma((world,)), dma((world,)), dma((world,)), dma((world,)), dma((world,)),
        ],
        compiler_params=pltpu.CompilerParams(has_side_effects=True, vmem_limit_bytes=48 << 20),
        cost_estimate=pl.CostEstimate(flops=100 * 10**9, bytes_accessed=40 << 20, transcendentals=0),
        name='dense_sums',
    )(acts_xn, acts_ao, dsend, gains, router)


def assemble_kernel(*refs):
    pieces, (qkv_ref, wo_ref, buf, in_sem, out_sem) = refs[:16], refs[16:]
    ep = lax.axis_index('ep')
    bits = (lax.rem(ep, 2), lax.rem(ep // 2, 2), ep // 4)
    size = HALF // 2
    width = buf.shape[2]
    split = width * 3 // 4

    def load(n):
        return pltpu.make_async_copy(pieces[n], buf.at[n % 4], in_sem.at[n % 4])

    def stores(n):
        flips = (n // 2 % 2, n // 4 % 2, n // 8)
        core, bx, by = [b + f - 2 * b * f for b, f in zip(bits, flips)]
        rows = pl.ds(pl.multiple_of(core * HALF + n % 2 * size, size), size)
        q = bx + 2 * by
        return [pltpu.make_async_copy(buf.at[n % 4, :, pl.ds(lo, cols)],
                                      ref.at[rows, pl.ds(pl.multiple_of(q * cols, 128), cols)], out_sem.at[n % 4, i])
                for i, (ref, lo, cols) in enumerate(((qkv_ref, 0, split), (wo_ref, split, width - split)))]

    for n in range(16 + 2):
        if n < 16:
            if n >= 4:
                for c in stores(n - 4):
                    c.wait()
            load(n).start()
        if n >= 2:
            load(n - 2).wait()
            for c in stores(n - 2):
                c.start()
    for n in range(12, 16):
        for c in stores(n):
            c.wait()


def assemble(pieces):
    width = pieces[0].shape[1]
    any_spec = pl.BlockSpec(memory_space=pl.ANY)
    return pl.pallas_call(
        assemble_kernel,
        out_shape=(jax.ShapeDtypeStruct((2 * HALF, 3 * width), F32), jax.ShapeDtypeStruct((2 * HALF, width), F32)),
        in_specs=[any_spec] * 16,
        out_specs=(any_spec, any_spec),
        scratch_shapes=[pltpu.VMEM((4, HALF // 2, width), F32), pltpu.SemaphoreType.DMA((4,)), pltpu.SemaphoreType.DMA((4, 2))],
        compiler_params=pltpu.CompilerParams(vmem_limit_bytes=24 << 20),
        cost_estimate=pl.CostEstimate(flops=20 * 10**9, bytes_accessed=80 << 20, transcendentals=0),
        name='assemble',
    )(*pieces)


def dot_nn(a, b):
    return lax.dot_general(a, b, (((1,), (0,)), ((), ())), preferred_element_type=jnp.float32)


def dot_nt(a, b):
    return lax.dot_general(a, b, (((1,), (1,)), ((), ())), preferred_element_type=jnp.float32)


def slot_select(codes_t, gates, first, local_exp, cap, codes_buf, gates_buf):
    tokens = codes_t.shape[1]
    codes_buf[...] = codes_t
    gates_buf[...] = gates
    my_codes = codes_buf[pl.ds(first, local_exp), :]
    my_gates = gates_buf[pl.ds(first, local_exp), :]
    slots = lax.broadcasted_iota(jnp.int32, (local_exp, cap, tokens), 1).astype(F32)
    select = jnp.where(my_codes[:, None, :] == slots, 1.0, 0.0)
    gate_slot = jnp.sum(select * my_gates[:, None, :], axis=-1, keepdims=True).reshape(local_exp * cap, 1)
    return select.reshape(local_exp * cap, tokens).astype(BF16), gate_slot


def slot_rows(xn, dyc, router, first, local_exp, cap, codes_buf, gates_buf):
    experts = router.shape[0]
    width = xn.shape[1]
    codes = dyc[:, width:].astype(F32).T[:experts]
    logits = dot_nt(router, xn)
    prob = jnp.exp(logits - jnp.max(logits, axis=0, keepdims=True))
    prob = prob / jnp.sum(prob, axis=0, keepdims=True)
    picked = jnp.where(codes < UNCHOSEN - 1.0, prob, 0.0)
    gates = picked / jnp.sum(picked, axis=0, keepdims=True)
    select, gate_slot = slot_select(codes, gates, first, local_exp, cap, codes_buf, gates_buf)
    return dot_nn(select, xn).astype(BF16), dot_nn(select, dyc[:, :width]), gate_slot


def dispatch_kernel(local_exp, cap, rows_ref, router_ref, recv_in, d_recv_in, recv_ref, d_recv_ref, codes_buf, gates_buf):
    first = pl.multiple_of(lax.axis_index('ep') * local_exp, local_exp)
    router = router_ref[...]
    width = router.shape[1]
    for i in range(rows_ref.shape[0]):
        recv, dy_rows, gate_slot = slot_rows(rows_ref[i, :, :width], rows_ref[i, :, width:], router, first, local_exp, cap,
                                             codes_buf.at[i], gates_buf.at[i])
        at = slice(i * cap, (i + 1) * cap)
        recv_ref[:, at, :] = recv.reshape(local_exp, cap, width)
        d_recv_ref[:, at, :] = (gate_slot * dy_rows).astype(BF16).reshape(local_exp, cap, width)


def dispatch_rows(rows, router_t, recv, d_recv, skip, cap):
    sources, tokens, lanes = rows.shape
    local_exp, _, width = recv.shape
    experts = router_t.shape[0]
    step = 4
    any_spec = pl.BlockSpec(memory_space=pl.ANY)
    out_spec = pl.BlockSpec((local_exp, step * cap, width), lambda s: (0, skip // (step * cap) + s, 0))
    same = lambda arr: jax.ShapeDtypeStruct(arr.shape, arr.dtype)
    return pl.pallas_call(
        functools.partial(dispatch_kernel, local_exp, cap),
        grid=(sources // step,),
        in_specs=[pl.BlockSpec((step, tokens, lanes), lambda s: (s, 0, 0)), pl.BlockSpec(router_t.shape, lambda s: (0, 0)), any_spec, any_spec],
        out_specs=(out_spec, out_spec),
        scratch_shapes=[pltpu.VMEM((step, experts, tokens), F32), pltpu.VMEM((step, experts, tokens), F32)],
        out_shape=(same(recv), same(d_recv)),
        input_output_aliases={2: 0, 3: 1},
        compiler_params=pltpu.CompilerParams(vmem_limit_bytes=56 << 20),
        cost_estimate=pl.CostEstimate(flops=sources * 4 * local_exp * cap * tokens * width, transcendentals=0,
                                      bytes_accessed=sources * tokens * width * 8),
        name='dispatch_rows',
    )(rows, router_t, recv, d_recv)


def hidden_grads(recv, d_recv, up, lin, down):
    u = dot_nn(recv, up).astype(BF16).astype(F32)
    v = dot_nn(recv, lin).astype(BF16).astype(F32)
    d_act = dot_nt(d_recv, down).astype(BF16).astype(F32)
    sig = jax.nn.sigmoid(u)
    act = u * sig
    d_u = d_act * v * (sig + act * (1.0 - sig))
    return (act * v).astype(BF16), d_u.astype(BF16), (d_act * act).astype(BF16)


def moe_kernel(cap, own_ref, router_ref, up_ref, lin_ref, down_ref, back_ref, gate_back_ref, recv_out, d_recv_out, hid_out,
               all_rows, recv, d_recv, dy_rows, d_tok, hid_buf, gate_send, up_buf, lin_buf, down_buf, codes_buf, gates_buf,
               w_sem, x_send, x_recv, p_send, p_recv, own_sem, row_sem, hid_sem, b_send, b_recv, g_send, g_recv):
    z = lax.axis_index('dp')
    ep = lax.axis_index('ep')
    local_exp = up_ref.shape[0]
    plane = all_rows.shape[0]
    width = router_ref.shape[1]
    first = pl.multiple_of(ep * local_exp, local_exp)
    bits = (lax.rem(ep, 2), lax.rem(ep // 2, 2), ep // 4)

    def flipped(d):
        flags = (lax.rem(d, 2), lax.rem(d // 2, 2), d // 4)
        both = [b + f - 2 * b * f for b, f in zip(bits, flags)]
        return both[0] + 2 * both[1] + 4 * both[2]

    def copy(src, dst, s_sem, r_sem, dev):
        return pltpu.make_async_remote_copy(src_ref=src, dst_ref=dst, send_sem=s_sem, recv_sem=r_sem,
                                            device_id=(z, dev), device_id_type=MESH)

    def weights(e, slot):
        return [pltpu.make_async_copy(src.at[e], dst.at[slot], w_sem.at[i, slot])
                for i, (src, dst) in enumerate(((up_ref, up_buf), (lin_ref, lin_buf), (down_ref, down_buf)))]

    for i in (1, 2):
        copy(own_ref, all_rows.at[ep], x_send.at[i], x_recv.at[i], flipped(2 * i)).start()
    copy(own_ref, all_rows.at[ep], p_send.at[0], p_recv.at[0], flipped(1)).start()
    part = pl.ds(0, own_ref.shape[0] // 2), pl.ds(own_ref.shape[0] // 2, own_ref.shape[0] // 2)

    def relay(n, src, dst):
        ref = all_rows.at[src, part[n], :]
        return copy(ref, ref, x_send.at[3 * n], x_recv.at[3 * n], dst)

    def share(i):
        ref = all_rows.at[flipped(2 * i)]
        return copy(ref, ref, p_send.at[i], p_recv.at[i], flipped(1))

    for c in weights(0, 0):
        c.start()
    all_rows[ep] = own_ref[...]
    router = router_ref[...]

    def pair(i, _):
        near = flipped(2 * i)
        other = flipped(2 * i + 1)

        @pl.when(i == 1)
        def _():
            for n in (1, 2):
                copy(own_ref, all_rows.at[flipped(2 * n)], x_send.at[n], x_recv.at[n], flipped(2 * n)).wait_recv()
                relay(n - 1, flipped(2 * n), flipped(6 - 2 * n)).start()
                share(n).start()

        @pl.when(i == 3)
        def _():
            relay(0, flipped(6), flipped(4)).wait_recv()
            relay(1, flipped(6), flipped(2)).wait_recv()
            share(3).start()

        copy(own_ref, all_rows.at[other], p_send.at[i], p_recv.at[i], flipped(1)).wait_recv()
        for j, src in enumerate((near, other)):
            rows, dy, gate_slot = slot_rows(all_rows[src, :, :width], all_rows[src, :, width:], router, first, local_exp, cap, codes_buf.at[j], gates_buf.at[j])
            at = pl.ds(pl.multiple_of(src * cap, cap), cap)
            recv[:, at, :] = rows.reshape(local_exp, cap, width)
            dy_rows[:, at, :] = dy.astype(BF16).reshape(local_exp, cap, width)
            d_recv[:, at, :] = (gate_slot * dy).astype(BF16).reshape(local_exp, cap, width)
        return 0

    lax.fori_loop(0, plane // 2, pair, 0)

    keep = [pltpu.make_async_copy(src, dst.at[:, pl.ds(0, plane * cap), :], row_sem.at[i])
            for i, (src, dst) in enumerate(((recv, recv_out), (d_recv, d_recv_out)))]
    for c in keep:
        c.start()

    def home(d, e):
        dev = flipped(d)
        src = d_tok.at[e, pl.ds(pl.multiple_of(dev * cap, cap), cap), :]
        return copy(src, back_ref.at[first + e], b_send.at[d, e], b_recv.at[d, e], dev)

    def stay(e):
        return pltpu.make_async_copy(d_tok.at[e, pl.ds(pl.multiple_of(ep * cap, cap), cap), :], back_ref.at[first + e], own_sem.at[e])

    def save(e):
        return pltpu.make_async_copy(hid_buf.at[lax.rem(e, 2)], hid_out.at[e], hid_sem.at[lax.rem(e, 2)])

    def expert(e, _):
        slot = lax.rem(e, 2)

        @pl.when(e + 1 < local_exp)
        def _():
            for c in weights(e + 1, 1 - slot):
                c.start()

        for c in weights(e, slot):
            c.wait()
        up, lin, down = up_buf[slot], lin_buf[slot], down_buf[slot]
        act, d_u, d_v = hidden_grads(recv[e], d_recv[e], up, lin, down)

        @pl.when(e >= 2)
        def _():
            save(e - 2).wait()

        for i, value in enumerate((act, d_u, d_v)):
            hid_buf[slot, i] = value
        d_tok[e] = (dot_nt(d_u, up) + dot_nt(d_v, lin)).astype(BF16)
        y = dot_nn(act, down).astype(BF16).astype(F32)
        d_gate = jnp.sum(dy_rows[e].astype(F32) * y, axis=-1, keepdims=True)
        lane = lax.broadcasted_iota(jnp.int32, (plane, cap, 128), 2)
        row = lax.broadcasted_iota(jnp.int32, (plane, cap, 128), 1)
        wide = jnp.broadcast_to(d_gate, (plane * cap, 128)).reshape(plane, cap, 128)
        gate_send[:, pl.ds(e, 1), :] = jnp.sum(jnp.where(lane == row, wide, 0.0), axis=1, keepdims=True)
        for d in (6, 7, 2, 3, 4, 5, 1):
            home(d, e).start()
        stay(e).start()
        save(e).start()
        return 0

    lax.fori_loop(0, local_exp, expert, 0)
    for e in (local_exp - 2, local_exp - 1):
        save(e).wait()

    for c in keep:
        c.wait()

    def gate_home(d):
        dev = flipped(d)
        return copy(gate_send.at[dev], gate_back_ref.at[ep], g_send.at[d], g_recv.at[d], dev)

    for d in range(1, plane):
        gate_home(d).start()
    gate_back_ref[ep] = gate_send[ep]

    def drain(e, _):
        for d in range(1, plane):
            src = d_tok.at[0, pl.ds(0, cap), :]
            copy(src, back_ref.at[flipped(d) * local_exp + e], b_send.at[d, e], b_recv.at[d, e], flipped(d)).wait_recv()
            home(d, e).wait_send()
        stay(e).wait()
        return 0

    lax.fori_loop(0, local_exp, drain, 0)
    for d in range(1, plane):
        copy(gate_send.at[0], gate_back_ref.at[flipped(d)], g_send.at[d], g_recv.at[d], flipped(d)).wait_recv()
        gate_home(d).wait_send()
    for i in (1, 2):
        copy(own_ref, all_rows.at[ep], x_send.at[i], x_recv.at[i], flipped(2 * i)).wait_send()
        relay(i - 1, flipped(2 * i), flipped(6 - 2 * i)).wait_send()
    for i in (1, 2, 3):
        share(i).wait_send()
    copy(own_ref, all_rows.at[ep], p_send.at[0], p_recv.at[0], flipped(1)).wait_send()


def moe_backward(rows_own, router_t, w_up, w_lin, w_down, cap, planes):
    tokens, lanes = rows_own.shape
    local_exp, width, hid = w_up.shape
    experts = router_t.shape[0]
    plane = experts // local_exp
    rows = pltpu.VMEM((local_exp, plane * cap, width), BF16)
    vmem = pl.BlockSpec(memory_space=pltpu.VMEM)
    any_spec = pl.BlockSpec(memory_space=pl.ANY)
    dma = pltpu.SemaphoreType.DMA
    return pl.pallas_call(
        functools.partial(moe_kernel, cap),
        out_shape=(jax.ShapeDtypeStruct((experts, cap, width), BF16), jax.ShapeDtypeStruct((plane, local_exp, 128), F32),
                   jax.ShapeDtypeStruct((local_exp, planes * plane * cap, width), BF16),
                   jax.ShapeDtypeStruct((local_exp, planes * plane * cap, width), BF16),
                   jax.ShapeDtypeStruct((local_exp, 3, plane * cap, hid), BF16)),
        in_specs=[vmem, vmem, any_spec, any_spec, any_spec],
        out_specs=(any_spec, vmem, any_spec, any_spec, any_spec),
        scratch_shapes=[
            pltpu.VMEM((plane, tokens, lanes), BF16), rows, rows, rows, rows, pltpu.VMEM((2, 3, plane * cap, hid), BF16), pltpu.VMEM((plane, local_exp, 128), F32),
            pltpu.VMEM((2, width, hid), BF16), pltpu.VMEM((2, width, hid), BF16), pltpu.VMEM((2, hid, width), BF16),
            pltpu.VMEM((2, experts, tokens), F32), pltpu.VMEM((2, experts, tokens), F32),
            dma((3, 2)), *[dma((4,))] * 4, dma((local_exp,)), dma((2,)), dma((2,)),
            dma((plane, local_exp)), dma((plane, local_exp)), dma((plane,)), dma((plane,)),
        ],
        compiler_params=pltpu.CompilerParams(has_side_effects=True, vmem_limit_bytes=60 << 20),
        cost_estimate=pl.CostEstimate(flops=60 * 10**9, bytes_accessed=64 << 20, transcendentals=0),
        name='moe_backward',
    )(rows_own, router_t, w_up, w_lin, w_down)


def weight_kernel(recv_ref, d_recv_ref, hid_ref, up_ref, lin_ref, down_ref, *rest):
    g_up_ref, g_lin_ref, g_down_ref, act_buf, du_buf, dv_buf = rest[-6:]
    total = recv_ref.shape[1]
    own = hid_ref.shape[2]
    for i, buf in enumerate((act_buf, du_buf, dv_buf)):
        buf[:own, :] = hid_ref[0, i]
    block = 256

    @pl.loop(own // block, total // block)
    def _(i):
        rows = pl.ds(pl.multiple_of(i * block, block), block)
        act, d_u, d_v = hidden_grads(recv_ref[0, rows, :], d_recv_ref[0, rows, :], up_ref[0], lin_ref[0], down_ref[0])
        act_buf[rows, :] = act
        du_buf[rows, :] = d_u
        dv_buf[rows, :] = d_v

    width = recv_ref.shape[2]
    cols = 512

    @pl.loop(0, width // cols)
    def _(i):
        c = pl.ds(pl.multiple_of(i * cols, cols), cols)
        g_up_ref[0, c, :] = dot_tn(recv_ref[0, :, c], du_buf[...])
        g_lin_ref[0, c, :] = dot_tn(recv_ref[0, :, c], dv_buf[...])
        g_down_ref[0, :, c] = dot_tn(act_buf[...], d_recv_ref[0, :, c])


def weight_grads(recv, d_recv, hid_own, w_up, w_lin, w_down, first, count, grads=()):
    _, total, width = recv.shape
    hid = w_up.shape[2]
    rows = pl.BlockSpec((1, total, width), lambda e: (first + e, 0, 0))
    wide = pl.BlockSpec((1, width, hid), lambda e: (first + e, 0, 0))
    tall = pl.BlockSpec((1, hid, width), lambda e: (first + e, 0, 0))
    f32 = lambda arr: jax.ShapeDtypeStruct(arr.shape, F32)
    return pl.pallas_call(
        weight_kernel,
        grid=(count,),
        out_shape=(f32(w_up), f32(w_lin), f32(w_down)),
        in_specs=[rows, rows, pl.BlockSpec((1,) + hid_own.shape[1:], lambda e: (first + e, 0, 0, 0)), wide, wide, tall]
        + [pl.BlockSpec(memory_space=pl.ANY)] * len(grads),
        out_specs=(wide, wide, tall),
        scratch_shapes=[pltpu.VMEM((total, hid), BF16)] * 3,
        input_output_aliases={6 + i: i for i in range(len(grads))},
        compiler_params=pltpu.CompilerParams(vmem_limit_bytes=60 << 20),
        cost_estimate=pl.CostEstimate(flops=12 * count * total * width * hid, transcendentals=0, bytes_accessed=count * (20 << 20)),
        name='weight_grads',
    )(recv, d_recv, hid_own, w_up, w_lin, w_down, *grads)


def solution(mesh):
    tok_spec = P(('dp', 'ep'))
    exp_spec = P('ep')
    rep_spec = P()

    def local(x_in, dy_in, route_idx, gain_attn, w_qkv, w_o, gain_ffn, w_router, w_up, w_lin, w_down):
        num_seqs, seq_len, width = x_in.shape
        tokens = num_seqs * seq_len
        top = route_idx.shape[-1]
        experts = w_router.shape[1]
        local_exp = w_up.shape[0]
        cap = ((tokens * top * 5) // (experts * 4) + 7) // 8 * 8
        ep_size = mesh.shape['ep']

        codes = slot_codes(route_idx.reshape(tokens, top), experts, cap)
        dy_own = dy_in.reshape(tokens, width)
        lanes = jnp.zeros((tokens, HEAD - experts), BF16)
        dyc_own = jnp.concatenate([dy_own, codes.T, lanes], axis=1)
        router_t = w_router.T
        planes = mesh.shape['dp']

        def spread(act):
            halves = jnp.moveaxis(act.reshape(tokens, 2, width // 2), 1, 0)
            send = jnp.broadcast_to(halves[None], (ep_size // 2, 2, tokens, width // 2)).reshape(ep_size, tokens, width // 2)
            return lax.all_to_all(send, 'ep', 0, 0).reshape(ep_size * tokens, width // 2)

        x_f = x_in.astype(F32)
        xn_one, norm_one_pull = jax.vjp(rms_norm, x_f, gain_attn.astype(F32))
        acts_xn = spread(xn_one)
        qkv_all = mm('bsd,de->bse', xn_one, w_qkv).astype(BF16)
        attn_out, attn_pull = jax.vjp(attn_core, qkv_all)
        attn_proj = mm('bsd,de->bse', attn_out, w_o)
        hidden = (x_f + attn_proj).astype(BF16).astype(F32).reshape(tokens, width)
        xn_two, norm_two_pull = jax.vjp(rms_norm, hidden, gain_ffn.astype(F32))

        rows_own = jnp.concatenate([xn_two, dyc_own], axis=1)
        foreign = [lax.ppermute(rows_own, 'dp', [((z + r) % planes, z) for z in range(planes)]) for r in range(1, planes)]
        d_back, gate_back, recv, d_recv, hid_own = moe_backward(rows_own, router_t, w_up, w_lin, w_down, cap, planes)
        acts_ao = spread(after(attn_out, gate_back))
        d_gate_back = gate_back[:, :, :cap].reshape(experts, cap)

        select_own = one_hot(codes, cap)
        d_moe_in = mm('ect,ecd->td', select_own, d_back)
        prob, mask, gates, total = gates_of(xn_two, codes, w_router)
        d_gates = jnp.sum(select_own.astype(F32) * d_gate_back[:, :, None], axis=1)
        d_picked = (d_gates - jnp.sum(d_gates * gates, axis=0, keepdims=True)) / total * mask
        d_logits = (prob * (d_picked - jnp.sum(prob * d_picked, axis=0, keepdims=True))).astype(BF16)
        d_xn_two = (d_moe_in + mm('et,de->td', d_logits, w_router)).astype(BF16)
        grad_router = mm('td,et->de', xn_two, d_logits)
        d_hidden, grad_gain_ffn = norm_two_pull(d_xn_two)
        d_resid = (d_hidden + dy_own.astype(F32)).astype(BF16).reshape(num_seqs, seq_len, width)
        d_attn_out = mm('bse,de->bsd', d_resid, w_o).astype(BF16)
        d_qkv = attn_pull(d_attn_out)[0]
        foreign = lax.all_gather(jnp.stack(foreign), 'ep')
        d_xn_one = mm('bse,de->bsd', d_qkv, w_qkv).astype(BF16)
        d_x_norm, grad_gain_attn = norm_one_pull(d_xn_one)
        dx_out = (d_x_norm + d_resid.astype(F32)).astype(BF16)
        quarters = lambda arr: jnp.moveaxis(arr.reshape(tokens, 4, -1), 1, 0)
        dsend = jnp.concatenate([quarters(d_qkv), quarters(d_resid)], axis=2)
        gains = jnp.concatenate([grad_gain_attn, grad_gain_ffn]).reshape(-1, 128)
        world_size = planes * ep_size
        low, high, gains, grad_router = dense_sums(acts_xn, acts_ao, dsend, gains, grad_router.reshape(world_size, -1, 128))
        grad_router = grad_router.reshape(width, experts)
        grad_gain_attn, grad_gain_ffn = gains.reshape(2, width)

        flip = lambda arr, bit: lax.ppermute(arr, 'ep', [(e, e ^ bit) for e in range(ep_size)])
        low_x, high_y = flip(low, 2), flip(high, 4)
        low_y, high_x = flip(low, 4), flip(high, 2)
        low_xy, high_xy = flip(low_x, 4), flip(high_y, 2)
        pieces = [low, high, low_x, high_x, low_y, high_y, low_xy, high_xy]
        swapped = [flip(arr, 1) for arr in pieces[:6]]
        swapped += [flip(arr, 1) for arr in pieces[6:]]
        pieces = [arr for i in range(4) for arr in (pieces[2 * i], pieces[2 * i + 1], swapped[2 * i], swapped[2 * i + 1])]

        foreign = after(foreign, gains)
        recv, d_recv = dispatch_rows(foreign.reshape(-1, tokens, foreign.shape[-1]), router_t, recv, d_recv, ep_size * cap, cap)
        grads, first = (), 0
        for count in (local_exp // 4, local_exp // 4, local_exp // 2):
            grads = weight_grads(recv, d_recv, hid_own, w_up, w_lin, w_down, first, count, grads)
            first += count
        grad_up, grad_lin, grad_down = grads
        grad_wqkv, grad_wo = assemble(pieces)
        return (dx_out, grad_gain_attn, grad_wqkv, grad_wo, grad_gain_ffn, grad_router, grad_up, grad_lin, grad_down)

    in_specs = (tok_spec, tok_spec, tok_spec, rep_spec, rep_spec, rep_spec, rep_spec, rep_spec, exp_spec, exp_spec, exp_spec)
    out_specs = (tok_spec, rep_spec, rep_spec, rep_spec, rep_spec, rep_spec, exp_spec, exp_spec, exp_spec)

    return jax.shard_map(local, mesh=mesh, in_specs=in_specs, out_specs=out_specs, check_vma=False)
```

```python
import functools

import jax
import jax.numpy as jnp
from jax import lax
from jax.experimental import pallas as pl
from jax.experimental.pallas import tpu as pltpu
from jax.sharding import PartitionSpec as P


EPS = 1e-6
HEAD = 128
DROPPED = 64.0
UNCHOSEN = 128.0
F32 = jnp.float32
BF16 = jnp.bfloat16


def mm(spec, a, b):
    return jnp.einsum(spec, a, b, preferred_element_type=F32)


def rms_norm(values, gain):
    scale = lax.rsqrt(jnp.mean(values * values, axis=-1, keepdims=True) + EPS)
    return (values * scale * gain).astype(BF16)


def attn_core(qkv_rows):
    num_seqs, seq_len, width = qkv_rows.shape
    heads = width // (3 * HEAD)
    split = qkv_rows.reshape(num_seqs, seq_len, 3, heads, HEAD)
    scores = mm('bqhc,bkhc->bhqk', split[:, :, 0], split[:, :, 1]) * (HEAD ** -0.5)
    rows = lax.broadcasted_iota(jnp.int32, (seq_len, seq_len), 0)
    cols = lax.broadcasted_iota(jnp.int32, (seq_len, seq_len), 1)
    scores = jnp.where(rows >= cols, scores, -1e30)
    prob_rows = jax.nn.softmax(scores, axis=-1).astype(BF16)
    mixed = mm('bhqk,bkhc->bqhc', prob_rows, split[:, :, 2])
    return mixed.astype(BF16).reshape(num_seqs, seq_len, heads * HEAD)


def slot_codes(idx_rows, experts, cap):
    tokens = idx_rows.shape[0]
    chosen = jnp.any(idx_rows[:, :, None] == jnp.arange(experts, dtype=jnp.int32), axis=1).astype(BF16)
    rows = lax.broadcasted_iota(jnp.int32, (tokens, tokens), 0)
    cols = lax.broadcasted_iota(jnp.int32, (tokens, tokens), 1)
    prior = mm('se,st->et', chosen, (rows < cols).astype(BF16))
    taken = mm('se,st->et', chosen, (rows == cols).astype(BF16))
    return jnp.where(taken > 0.5, jnp.where(prior < cap, prior, DROPPED), UNCHOSEN).astype(BF16)


def one_hot(codes, cap):
    slots = lax.broadcasted_iota(jnp.int32, codes.shape[:-1] + (cap, codes.shape[-1]), codes.ndim - 1)
    return (codes[..., None, :].astype(F32) == slots.astype(F32)).astype(BF16)


def gates_of(xn, codes, w_router):
    logits = mm('...td,de->...et', xn, w_router)
    prob = jax.nn.softmax(logits, axis=-2)
    mask = (codes.astype(F32) < UNCHOSEN - 1.0).astype(F32)
    picked = prob * mask
    total = jnp.sum(picked, axis=-2, keepdims=True)
    return prob, mask, picked / total, total


def after(value, *deps):
    return lax.optimization_barrier((value,) + deps)[0]


HALF = 768
CHUNK = 64
STEPS = HALF // CHUNK
BLOCK = 128
MESH = pl.DeviceIdType.MESH


def dot_tn(a, b):
    return lax.dot_general(a, b, (((0,), (0,)), ((), ())), preferred_element_type=jnp.float32)


def dense_kernel(acts_xn_ref, acts_ao_ref, dsend_ref, gains_ref, router_ref, low_ref, high_ref, gains_out_ref, router_out_ref,
                 dall, stage, part, z_in, total, gain_buf, router_buf,
                 d_send, d_recv, h_send, h_recv, o_send, o_recv, dp_send, dp_recv, z_send, z_recv, own_sem,
                 g_send, g_recv, r_send, r_recv, s_send, s_recv):
    z = lax.axis_index('dp')
    ep = lax.axis_index('ep')
    core = lax.rem(ep, 2)
    quarter = ep // 2
    width = dsend_ref.shape[2]
    split = width * 3 // 4
    tokens = dsend_ref.shape[1]
    partner = ep + 1 - 2 * core
    bit_x = lax.rem(quarter, 2)
    bit_y = quarter // 2
    flip = lambda bx, by: 2 * ((bit_x + bx - 2 * bit_x * bx) + 2 * (bit_y + by - 2 * bit_y * by)) + core
    x_dev, y_dev, xy_dev = flip(1, 0), flip(0, 1), flip(1, 1)
    inner = jnp.logical_or(z == 1, z == 2)
    z_mate = jnp.where(z == 0, 1, jnp.where(z == 1, 0, jnp.where(z == 2, 3, 2)))
    z_cross = 3 - z

    def copy(src, dst, s_sem, r_sem, dp, e):
        return pltpu.make_async_remote_copy(src_ref=src, dst_ref=dst, send_sem=s_sem, recv_sem=r_sem,
                                            device_id=(dp, e), device_id_type=MESH)

    rows_of = lambda e: pl.ds(pl.multiple_of(e * tokens, tokens), tokens)
    far = (x_dev, y_dev, xy_dev)
    halves = pl.ds(0, tokens // 2), pl.ds(tokens // 2, tokens // 2)
    direct = lambda i: copy(dsend_ref.at[far[i] // 2], dall.at[rows_of(ep)], d_send.at[i], d_recv.at[i], z, far[i])
    hop = lambda n: copy(dsend_ref.at[xy_dev // 2, halves[n], :], stage.at[n], h_send.at[n], h_recv.at[n], z, far[n])

    def onward(n):
        at = pl.ds(pl.multiple_of(far[n] * tokens + n * (tokens // 2), tokens // 2), tokens // 2)
        return copy(stage.at[n], dall.at[at], o_send.at[n], o_recv.at[n], z, far[1 - n])

    def landed(n):
        at = pl.ds(pl.multiple_of(xy_dev * tokens + n * (tokens // 2), tokens // 2), tokens // 2)
        return copy(stage.at[n], dall.at[at], o_send.at[n], o_recv.at[n], z, far[1 - n])

    for n in range(2):
        hop(n).start()
    for i in range(2):
        direct(i).start()
    copy(dsend_ref.at[quarter], dall.at[rows_of(ep)], dp_send.at[3], dp_recv.at[3], z, partner).start()

    world = router_ref.shape[0]
    me = z * 8 + ep

    def push(pick, buf, s_sem, r_sem, d, target):
        return copy(pick(target), buf.at[me], s_sem.at[d], r_sem.at[d], target // 8, lax.rem(target, 8))

    def push_all(*args):
        def body(d, _):
            push(*args, d, lax.rem(me + d, world)).start()
            return _

        lax.fori_loop(1, world, body, 0)

    def wait_all(pick, buf, s_sem, r_sem):
        def body(d, _):
            push(pick, buf, s_sem, r_sem, d, lax.rem(me + d, world)).wait()
            return _

        lax.fori_loop(1, world, body, 0)

    def device_sum(buf):
        return lax.fori_loop(0, world, lambda s, acc: acc + buf[s], jnp.zeros(buf.shape[1:], jnp.float32))

    gain_push = (lambda t: gains_ref, gain_buf, g_send, g_recv)
    share_push = (lambda t: router_ref.at[t], router_buf, r_send, r_recv)
    total_push = (lambda t: router_out_ref.at[me], router_out_ref, s_send, s_recv)
    push_all(*gain_push)
    push_all(*share_push)

    dall[rows_of(ep), :] = dsend_ref[quarter]
    to_core = lambda i: copy(dall.at[rows_of(far[i])], dall.at[rows_of(far[i])], dp_send.at[i], dp_recv.at[i], z, partner)
    for n in range(2):
        hop(n).wait_recv()
        onward(n).start()
    for i in range(2):
        copy(dsend_ref.at[0], dall.at[rows_of(far[i])], d_send.at[i], d_recv.at[i], z, far[i]).wait_recv()
        to_core(i).start()
    for n in range(2):
        landed(n).wait_recv()
    to_core(2).start()
    for i, dev in enumerate(far + (ep,)):
        other = dev + 1 - 2 * core
        copy(dsend_ref.at[0], dall.at[rows_of(other)], dp_send.at[i], dp_recv.at[i], z, partner).wait_recv()

    up_copy = lambda k: copy(part.at[k], z_in.at[k], z_send.at[0, k], z_recv.at[0, k], z_mate, ep)
    cross_copy = lambda k: copy(part.at[k], total.at[k], z_send.at[1, k], z_recv.at[1, k], z_cross, ep)
    down_copy = lambda k: copy(total.at[k], total.at[k], z_send.at[2, k], z_recv.at[2, k], z_mate, ep)

    def own_copy(k):
        ref = low_ref if k < STEPS // 2 else high_ref
        return pltpu.make_async_copy(total.at[k], ref.at[pl.ds(k % (STEPS // 2) * CHUNK, CHUNK), :], own_sem.at[k])

    for i in range(STEPS + 7):
        k = i
        if k < STEPS and k * CHUNK % BLOCK == 0:
            cols = slice(k * CHUNK, k * CHUNK + BLOCK)
            many = BLOCK // CHUNK
            part[k:k + many, :, :split] = dot_tn(acts_xn_ref[:, cols], dall[:, :split]).reshape(many, CHUNK, split)
            part[k:k + many, :, split:] = dot_tn(acts_ao_ref[:, cols], dall[:, split:]).reshape(many, CHUNK, width - split)
        if i == 6:
            wait_all(*share_push)
            router_buf[me] = router_ref[me]
            router_out_ref[me] = device_sum(router_buf)
        if i == 8:
            push_all(*total_push)
        a = i - 1
        t = i - 3

        @pl.when(inner)
        def _():
            if 0 <= a < STEPS:
                up_copy(a).wait_recv()
                part[a] = part[a] + z_in[a]
                cross_copy(a).start()
            if 0 <= t < STEPS:
                cross_copy(t).wait_recv()
                total[t] = part[t] + total[t]
                down_copy(t).start()
                own_copy(t).start()

        @pl.when(jnp.logical_not(inner))
        def _():
            if k < STEPS:
                up_copy(k).start()
            if 0 <= i - 7 < STEPS:
                down_copy(i - 7).wait_recv()
                own_copy(i - 7).start()

    for k in range(STEPS):
        own_copy(k).wait()

    @pl.when(inner)
    def _():
        for k in range(STEPS):
            cross_copy(k).wait_send()
            down_copy(k).wait_send()

    @pl.when(jnp.logical_not(inner))
    def _():
        for k in range(STEPS):
            up_copy(k).wait_send()

    for n in range(2):
        direct(n).wait_send()
        hop(n).wait_send()
        onward(n).wait_send()
    for i in range(3):
        to_core(i).wait_send()
    copy(dsend_ref.at[quarter], dall.at[rows_of(ep)], dp_send.at[3], dp_recv.at[3], z, partner).wait_send()

    wait_all(*gain_push)
    gain_buf[me] = gains_ref[...]
    gains_out_ref[...] = device_sum(gain_buf)
    wait_all(*total_push)


def dense_sums(acts_xn, acts_ao, dsend, gains, router):
    rows, width = acts_xn.shape[0], dsend.shape[2]
    any_spec = pl.BlockSpec(memory_space=pl.ANY)
    vmem = pl.BlockSpec(memory_space=pltpu.VMEM)
    dma = pltpu.SemaphoreType.DMA
    f32 = lambda *shape: jax.ShapeDtypeStruct(shape, jnp.float32)
    world = router.shape[0]
    return pl.pallas_call(
        dense_kernel,
        out_shape=(f32(HALF // 2, width), f32(HALF // 2, width), f32(*gains.shape), f32(*router.shape)),
        in_specs=[vmem, vmem, vmem, vmem, vmem],
        out_specs=(any_spec, any_spec, vmem, vmem),
        scratch_shapes=[
            pltpu.VMEM((rows, width), jnp.bfloat16),
            pltpu.VMEM((2, dsend.shape[1] // 2, width), jnp.bfloat16),
            pltpu.VMEM((STEPS, CHUNK, width), jnp.float32),
            pltpu.VMEM((STEPS, CHUNK, width), jnp.float32),
            pltpu.VMEM((STEPS, CHUNK, width), jnp.float32),
            pltpu.VMEM((world,) + gains.shape, jnp.float32),
            pltpu.VMEM(router.shape, jnp.float32),
            *[dma((2,))] * 6, *[dma((4,))] * 2, dma((3, STEPS)), dma((3, STEPS)), dma((STEPS,)),
            dma((world,)), dma((world,)), dma((world,)), dma((world,)), dma((world,)), dma((world,)),
        ],
        compiler_params=pltpu.CompilerParams(has_side_effects=True, vmem_limit_bytes=48 << 20),
        cost_estimate=pl.CostEstimate(flops=100 * 10**9, bytes_accessed=40 << 20, transcendentals=0),
        name='dense_sums',
    )(acts_xn, acts_ao, dsend, gains, router)


def assemble_kernel(*refs):
    pieces, (qkv_ref, wo_ref, buf, in_sem, out_sem) = refs[:16], refs[16:]
    ep = lax.axis_index('ep')
    bits = (lax.rem(ep, 2), lax.rem(ep // 2, 2), ep // 4)
    size = HALF // 2
    width = buf.shape[2]
    split = width * 3 // 4

    def load(n):
        return pltpu.make_async_copy(pieces[n], buf.at[n % 4], in_sem.at[n % 4])

    def stores(n):
        flips = (n // 2 % 2, n // 4 % 2, n // 8)
        core, bx, by = [b + f - 2 * b * f for b, f in zip(bits, flips)]
        rows = pl.ds(pl.multiple_of(core * HALF + n % 2 * size, size), size)
        q = bx + 2 * by
        return [pltpu.make_async_copy(buf.at[n % 4, :, pl.ds(lo, cols)],
                                      ref.at[rows, pl.ds(pl.multiple_of(q * cols, 128), cols)], out_sem.at[n % 4, i])
                for i, (ref, lo, cols) in enumerate(((qkv_ref, 0, split), (wo_ref, split, width - split)))]

    for n in range(16 + 2):
        if n < 16:
            if n >= 4:
                for c in stores(n - 4):
                    c.wait()
            load(n).start()
        if n >= 2:
            load(n - 2).wait()
            for c in stores(n - 2):
                c.start()
    for n in range(12, 16):
        for c in stores(n):
            c.wait()


def assemble(pieces):
    width = pieces[0].shape[1]
    any_spec = pl.BlockSpec(memory_space=pl.ANY)
    return pl.pallas_call(
        assemble_kernel,
        out_shape=(jax.ShapeDtypeStruct((2 * HALF, 3 * width), F32), jax.ShapeDtypeStruct((2 * HALF, width), F32)),
        in_specs=[any_spec] * 16,
        out_specs=(any_spec, any_spec),
        scratch_shapes=[pltpu.VMEM((4, HALF // 2, width), F32), pltpu.SemaphoreType.DMA((4,)), pltpu.SemaphoreType.DMA((4, 2))],
        compiler_params=pltpu.CompilerParams(vmem_limit_bytes=24 << 20),
        cost_estimate=pl.CostEstimate(flops=20 * 10**9, bytes_accessed=80 << 20, transcendentals=0),
        name='assemble',
    )(*pieces)


def dot_nn(a, b):
    return lax.dot_general(a, b, (((1,), (0,)), ((), ())), preferred_element_type=jnp.float32)


def dot_nt(a, b):
    return lax.dot_general(a, b, (((1,), (1,)), ((), ())), preferred_element_type=jnp.float32)


def slot_select(codes_t, gates, first, local_exp, cap, codes_buf, gates_buf):
    tokens = codes_t.shape[1]
    codes_buf[...] = codes_t
    gates_buf[...] = gates
    my_codes = codes_buf[pl.ds(first, local_exp), :]
    my_gates = gates_buf[pl.ds(first, local_exp), :]
    slots = lax.broadcasted_iota(jnp.int32, (local_exp, cap, tokens), 1).astype(F32)
    select = jnp.where(my_codes[:, None, :] == slots, 1.0, 0.0)
    gate_slot = jnp.sum(select * my_gates[:, None, :], axis=-1, keepdims=True).reshape(local_exp * cap, 1)
    return select.reshape(local_exp * cap, tokens).astype(BF16), gate_slot


def slot_rows(xn, dyc, router, first, local_exp, cap, codes_buf, gates_buf):
    experts = router.shape[0]
    width = xn.shape[1]
    codes = dyc[:, width:].astype(F32).T[:experts]
    logits = dot_nt(router, xn)
    prob = jnp.exp(logits - jnp.max(logits, axis=0, keepdims=True))
    prob = prob / jnp.sum(prob, axis=0, keepdims=True)
    picked = jnp.where(codes < UNCHOSEN - 1.0, prob, 0.0)
    gates = picked / jnp.sum(picked, axis=0, keepdims=True)
    select, gate_slot = slot_select(codes, gates, first, local_exp, cap, codes_buf, gates_buf)
    return dot_nn(select, xn).astype(BF16), dot_nn(select, dyc[:, :width]), gate_slot


def dispatch_kernel(local_exp, cap, rows_ref, router_ref, recv_in, d_recv_in, recv_ref, d_recv_ref, codes_buf, gates_buf):
    first = pl.multiple_of(lax.axis_index('ep') * local_exp, local_exp)
    router = router_ref[...]
    width = router.shape[1]
    for i in range(rows_ref.shape[0]):
        recv, dy_rows, gate_slot = slot_rows(rows_ref[i, :, :width], rows_ref[i, :, width:], router, first, local_exp, cap,
                                             codes_buf.at[i], gates_buf.at[i])
        at = slice(i * cap, (i + 1) * cap)
        recv_ref[:, at, :] = recv.reshape(local_exp, cap, width)
        d_recv_ref[:, at, :] = (gate_slot * dy_rows).astype(BF16).reshape(local_exp, cap, width)


def dispatch_rows(rows, router_t, recv, d_recv, skip, cap):
    sources, tokens, lanes = rows.shape
    local_exp, _, width = recv.shape
    experts = router_t.shape[0]
    step = 4
    any_spec = pl.BlockSpec(memory_space=pl.ANY)
    out_spec = pl.BlockSpec((local_exp, step * cap, width), lambda s: (0, skip // (step * cap) + s, 0))
    same = lambda arr: jax.ShapeDtypeStruct(arr.shape, arr.dtype)
    return pl.pallas_call(
        functools.partial(dispatch_kernel, local_exp, cap),
        grid=(sources // step,),
        in_specs=[pl.BlockSpec((step, tokens, lanes), lambda s: (s, 0, 0)), pl.BlockSpec(router_t.shape, lambda s: (0, 0)), any_spec, any_spec],
        out_specs=(out_spec, out_spec),
        scratch_shapes=[pltpu.VMEM((step, experts, tokens), F32), pltpu.VMEM((step, experts, tokens), F32)],
        out_shape=(same(recv), same(d_recv)),
        input_output_aliases={2: 0, 3: 1},
        compiler_params=pltpu.CompilerParams(vmem_limit_bytes=56 << 20),
        cost_estimate=pl.CostEstimate(flops=sources * 4 * local_exp * cap * tokens * width, transcendentals=0,
                                      bytes_accessed=sources * tokens * width * 8),
        name='dispatch_rows',
    )(rows, router_t, recv, d_recv)


def hidden_grads(recv, d_recv, up, lin, down):
    u = dot_nn(recv, up).astype(BF16).astype(F32)
    v = dot_nn(recv, lin).astype(BF16).astype(F32)
    d_act = dot_nt(d_recv, down).astype(BF16).astype(F32)
    sig = jax.nn.sigmoid(u)
    act = u * sig
    d_u = d_act * v * (sig + act * (1.0 - sig))
    return (act * v).astype(BF16), d_u.astype(BF16), (d_act * act).astype(BF16)


def moe_kernel(cap, own_ref, router_ref, up_ref, lin_ref, down_ref, back_ref, gate_back_ref, recv_out, d_recv_out, hid_out,
               all_rows, recv, d_recv, dy_rows, d_tok, hid_buf, gate_send, up_buf, lin_buf, down_buf, codes_buf, gates_buf,
               w_sem, x_send, x_recv, p_send, p_recv, own_sem, row_sem, hid_sem, b_send, b_recv, g_send, g_recv):
    z = lax.axis_index('dp')
    ep = lax.axis_index('ep')
    local_exp = up_ref.shape[0]
    plane = all_rows.shape[0]
    width = router_ref.shape[1]
    first = pl.multiple_of(ep * local_exp, local_exp)
    bits = (lax.rem(ep, 2), lax.rem(ep // 2, 2), ep // 4)

    def flipped(d):
        flags = (lax.rem(d, 2), lax.rem(d // 2, 2), d // 4)
        both = [b + f - 2 * b * f for b, f in zip(bits, flags)]
        return both[0] + 2 * both[1] + 4 * both[2]

    def copy(src, dst, s_sem, r_sem, dev):
        return pltpu.make_async_remote_copy(src_ref=src, dst_ref=dst, send_sem=s_sem, recv_sem=r_sem,
                                            device_id=(z, dev), device_id_type=MESH)

    def weights(e, slot):
        return [pltpu.make_async_copy(src.at[e], dst.at[slot], w_sem.at[i, slot])
                for i, (src, dst) in enumerate(((up_ref, up_buf), (lin_ref, lin_buf), (down_ref, down_buf)))]

    for i in (1, 2):
        copy(own_ref, all_rows.at[ep], x_send.at[i], x_recv.at[i], flipped(2 * i)).start()
    copy(own_ref, all_rows.at[ep], p_send.at[0], p_recv.at[0], flipped(1)).start()
    part = pl.ds(0, own_ref.shape[0] // 2), pl.ds(own_ref.shape[0] // 2, own_ref.shape[0] // 2)

    def relay(n, src, dst):
        ref = all_rows.at[src, part[n], :]
        return copy(ref, ref, x_send.at[3 * n], x_recv.at[3 * n], dst)

    def share(i):
        ref = all_rows.at[flipped(2 * i)]
        return copy(ref, ref, p_send.at[i], p_recv.at[i], flipped(1))

    for c in weights(0, 0):
        c.start()
    all_rows[ep] = own_ref[...]
    router = router_ref[...]

    def pair(i, _):
        near = flipped(2 * i)
        other = flipped(2 * i + 1)

        @pl.when(i == 1)
        def _():
            for n in (1, 2):
                copy(own_ref, all_rows.at[flipped(2 * n)], x_send.at[n], x_recv.at[n], flipped(2 * n)).wait_recv()
                relay(n - 1, flipped(2 * n), flipped(6 - 2 * n)).start()
                share(n).start()

        @pl.when(i == 3)
        def _():
            relay(0, flipped(6), flipped(4)).wait_recv()
            relay(1, flipped(6), flipped(2)).wait_recv()
            share(3).start()

        copy(own_ref, all_rows.at[other], p_send.at[i], p_recv.at[i], flipped(1)).wait_recv()
        for j, src in enumerate((near, other)):
            rows, dy, gate_slot = slot_rows(all_rows[src, :, :width], all_rows[src, :, width:], router, first, local_exp, cap, codes_buf.at[j], gates_buf.at[j])
            at = pl.ds(pl.multiple_of(src * cap, cap), cap)
            recv[:, at, :] = rows.reshape(local_exp, cap, width)
            dy_rows[:, at, :] = dy.astype(BF16).reshape(local_exp, cap, width)
            d_recv[:, at, :] = (gate_slot * dy).astype(BF16).reshape(local_exp, cap, width)
        return 0

    lax.fori_loop(0, plane // 2, pair, 0)

    keep = [pltpu.make_async_copy(src, dst.at[:, pl.ds(0, plane * cap), :], row_sem.at[i])
            for i, (src, dst) in enumerate(((recv, recv_out), (d_recv, d_recv_out)))]
    for c in keep:
        c.start()

    def home(d, e):
        dev = flipped(d)
        src = d_tok.at[e, pl.ds(pl.multiple_of(dev * cap, cap), cap), :]
        return copy(src, back_ref.at[first + e], b_send.at[d, e], b_recv.at[d, e], dev)

    def stay(e):
        return pltpu.make_async_copy(d_tok.at[e, pl.ds(pl.multiple_of(ep * cap, cap), cap), :], back_ref.at[first + e], own_sem.at[e])

    def save(e):
        return pltpu.make_async_copy(hid_buf.at[lax.rem(e, 2)], hid_out.at[e], hid_sem.at[lax.rem(e, 2)])

    def expert(e, _):
        slot = lax.rem(e, 2)

        @pl.when(e + 1 < local_exp)
        def _():
            for c in weights(e + 1, 1 - slot):
                c.start()

        for c in weights(e, slot):
            c.wait()
        up, lin, down = up_buf[slot], lin_buf[slot], down_buf[slot]
        act, d_u, d_v = hidden_grads(recv[e], d_recv[e], up, lin, down)

        @pl.when(e >= 2)
        def _():
            save(e - 2).wait()

        for i, value in enumerate((act, d_u, d_v)):
            hid_buf[slot, i] = value
        d_tok[e] = (dot_nt(d_u, up) + dot_nt(d_v, lin)).astype(BF16)
        y = dot_nn(act, down).astype(BF16).astype(F32)
        d_gate = jnp.sum(dy_rows[e].astype(F32) * y, axis=-1, keepdims=True)
        lane = lax.broadcasted_iota(jnp.int32, (plane, cap, 128), 2)
        row = lax.broadcasted_iota(jnp.int32, (plane, cap, 128), 1)
        wide = jnp.broadcast_to(d_gate, (plane * cap, 128)).reshape(plane, cap, 128)
        gate_send[:, pl.ds(e, 1), :] = jnp.sum(jnp.where(lane == row, wide, 0.0), axis=1, keepdims=True)
        for d in (6, 7, 2, 3, 4, 5, 1):
            home(d, e).start()
        stay(e).start()
        save(e).start()
        return 0

    lax.fori_loop(0, local_exp, expert, 0)
    for e in (local_exp - 2, local_exp - 1):
        save(e).wait()

    for c in keep:
        c.wait()

    def gate_home(d):
        dev = flipped(d)
        return copy(gate_send.at[dev], gate_back_ref.at[ep], g_send.at[d], g_recv.at[d], dev)

    for d in range(1, plane):
        gate_home(d).start()
    gate_back_ref[ep] = gate_send[ep]

    def drain(e, _):
        for d in range(1, plane):
            src = d_tok.at[0, pl.ds(0, cap), :]
            copy(src, back_ref.at[flipped(d) * local_exp + e], b_send.at[d, e], b_recv.at[d, e], flipped(d)).wait_recv()
            home(d, e).wait_send()
        stay(e).wait()
        return 0

    lax.fori_loop(0, local_exp, drain, 0)
    for d in range(1, plane):
        copy(gate_send.at[0], gate_back_ref.at[flipped(d)], g_send.at[d], g_recv.at[d], flipped(d)).wait_recv()
        gate_home(d).wait_send()
    for i in (1, 2):
        copy(own_ref, all_rows.at[ep], x_send.at[i], x_recv.at[i], flipped(2 * i)).wait_send()
        relay(i - 1, flipped(2 * i), flipped(6 - 2 * i)).wait_send()
    for i in (1, 2, 3):
        share(i).wait_send()
    copy(own_ref, all_rows.at[ep], p_send.at[0], p_recv.at[0], flipped(1)).wait_send()


def moe_backward(rows_own, router_t, w_up, w_lin, w_down, cap, planes):
    tokens, lanes = rows_own.shape
    local_exp, width, hid = w_up.shape
    experts = router_t.shape[0]
    plane = experts // local_exp
    rows = pltpu.VMEM((local_exp, plane * cap, width), BF16)
    vmem = pl.BlockSpec(memory_space=pltpu.VMEM)
    any_spec = pl.BlockSpec(memory_space=pl.ANY)
    dma = pltpu.SemaphoreType.DMA
    return pl.pallas_call(
        functools.partial(moe_kernel, cap),
        out_shape=(jax.ShapeDtypeStruct((experts, cap, width), BF16), jax.ShapeDtypeStruct((plane, local_exp, 128), F32),
                   jax.ShapeDtypeStruct((local_exp, planes * plane * cap, width), BF16),
                   jax.ShapeDtypeStruct((local_exp, planes * plane * cap, width), BF16),
                   jax.ShapeDtypeStruct((local_exp, 3, plane * cap, hid), BF16)),
        in_specs=[vmem, vmem, any_spec, any_spec, any_spec],
        out_specs=(any_spec, vmem, any_spec, any_spec, any_spec),
        scratch_shapes=[
            pltpu.VMEM((plane, tokens, lanes), BF16), rows, rows, rows, rows, pltpu.VMEM((2, 3, plane * cap, hid), BF16), pltpu.VMEM((plane, local_exp, 128), F32),
            pltpu.VMEM((2, width, hid), BF16), pltpu.VMEM((2, width, hid), BF16), pltpu.VMEM((2, hid, width), BF16),
            pltpu.VMEM((2, experts, tokens), F32), pltpu.VMEM((2, experts, tokens), F32),
            dma((3, 2)), *[dma((4,))] * 4, dma((local_exp,)), dma((2,)), dma((2,)),
            dma((plane, local_exp)), dma((plane, local_exp)), dma((plane,)), dma((plane,)),
        ],
        compiler_params=pltpu.CompilerParams(has_side_effects=True, vmem_limit_bytes=60 << 20),
        cost_estimate=pl.CostEstimate(flops=60 * 10**9, bytes_accessed=64 << 20, transcendentals=0),
        name='moe_backward',
    )(rows_own, router_t, w_up, w_lin, w_down)


def weight_kernel(recv_ref, d_recv_ref, hid_ref, up_ref, lin_ref, down_ref, *rest):
    g_up_ref, g_lin_ref, g_down_ref, act_buf, du_buf, dv_buf = rest[-6:]
    total = recv_ref.shape[1]
    own = hid_ref.shape[2]
    for i, buf in enumerate((act_buf, du_buf, dv_buf)):
        buf[:own, :] = hid_ref[0, i]
    block = 256

    @pl.loop(own // block, total // block)
    def _(i):
        rows = pl.ds(pl.multiple_of(i * block, block), block)
        act, d_u, d_v = hidden_grads(recv_ref[0, rows, :], d_recv_ref[0, rows, :], up_ref[0], lin_ref[0], down_ref[0])
        act_buf[rows, :] = act
        du_buf[rows, :] = d_u
        dv_buf[rows, :] = d_v

    width = recv_ref.shape[2]
    cols = 512

    @pl.loop(0, width // cols)
    def _(i):
        c = pl.ds(pl.multiple_of(i * cols, cols), cols)
        g_up_ref[0, c, :] = dot_tn(recv_ref[0, :, c], du_buf[...])
        g_lin_ref[0, c, :] = dot_tn(recv_ref[0, :, c], dv_buf[...])
        g_down_ref[0, :, c] = dot_tn(act_buf[...], d_recv_ref[0, :, c])


def weight_grads(recv, d_recv, hid_own, w_up, w_lin, w_down, first, count, grads=()):
    _, total, width = recv.shape
    hid = w_up.shape[2]
    rows = pl.BlockSpec((1, total, width), lambda e: (first + e, 0, 0))
    wide = pl.BlockSpec((1, width, hid), lambda e: (first + e, 0, 0))
    tall = pl.BlockSpec((1, hid, width), lambda e: (first + e, 0, 0))
    f32 = lambda arr: jax.ShapeDtypeStruct(arr.shape, F32)
    return pl.pallas_call(
        weight_kernel,
        grid=(count,),
        out_shape=(f32(w_up), f32(w_lin), f32(w_down)),
        in_specs=[rows, rows, pl.BlockSpec((1,) + hid_own.shape[1:], lambda e: (first + e, 0, 0, 0)), wide, wide, tall]
        + [pl.BlockSpec(memory_space=pl.ANY)] * len(grads),
        out_specs=(wide, wide, tall),
        scratch_shapes=[pltpu.VMEM((total, hid), BF16)] * 3,
        input_output_aliases={6 + i: i for i in range(len(grads))},
        compiler_params=pltpu.CompilerParams(vmem_limit_bytes=60 << 20),
        cost_estimate=pl.CostEstimate(flops=12 * count * total * width * hid, transcendentals=0, bytes_accessed=count * (20 << 20)),
        name='weight_grads',
    )(recv, d_recv, hid_own, w_up, w_lin, w_down, *grads)


def solution(mesh):
    tok_spec = P(('dp', 'ep'))
    exp_spec = P('ep')
    rep_spec = P()

    def local(x_in, dy_in, route_idx, gain_attn, w_qkv, w_o, gain_ffn, w_router, w_up, w_lin, w_down):
        num_seqs, seq_len, width = x_in.shape
        tokens = num_seqs * seq_len
        top = route_idx.shape[-1]
        experts = w_router.shape[1]
        local_exp = w_up.shape[0]
        cap = ((tokens * top * 5) // (experts * 4) + 7) // 8 * 8
        ep_size = mesh.shape['ep']

        codes = slot_codes(route_idx.reshape(tokens, top), experts, cap)
        dy_own = dy_in.reshape(tokens, width)
        lanes = jnp.zeros((tokens, HEAD - experts), BF16)
        dyc_own = jnp.concatenate([dy_own, codes.T, lanes], axis=1)
        router_t = w_router.T
        planes = mesh.shape['dp']

        def spread(act):
            halves = jnp.moveaxis(act.reshape(tokens, 2, width // 2), 1, 0)
            send = jnp.broadcast_to(halves[None], (ep_size // 2, 2, tokens, width // 2)).reshape(ep_size, tokens, width // 2)
            return lax.all_to_all(send, 'ep', 0, 0).reshape(ep_size * tokens, width // 2)

        x_f = x_in.astype(F32)
        xn_one, norm_one_pull = jax.vjp(rms_norm, x_f, gain_attn.astype(F32))
        acts_xn = spread(xn_one)
        qkv_all = mm('bsd,de->bse', xn_one, w_qkv).astype(BF16)
        attn_out, attn_pull = jax.vjp(attn_core, qkv_all)
        attn_proj = mm('bsd,de->bse', attn_out, w_o)
        hidden = (x_f + attn_proj).astype(BF16).astype(F32).reshape(tokens, width)
        xn_two, norm_two_pull = jax.vjp(rms_norm, hidden, gain_ffn.astype(F32))

        rows_own = jnp.concatenate([xn_two, dyc_own], axis=1)
        foreign = [lax.ppermute(rows_own, 'dp', [((z + r) % planes, z) for z in range(planes)]) for r in range(1, planes)]
        d_back, gate_back, recv, d_recv, hid_own = moe_backward(rows_own, router_t, w_up, w_lin, w_down, cap, planes)
        acts_ao = spread(after(attn_out, gate_back))
        d_gate_back = gate_back[:, :, :cap].reshape(experts, cap)

        select_own = one_hot(codes, cap)
        d_moe_in = mm('ect,ecd->td', select_own, d_back)
        prob, mask, gates, total = gates_of(xn_two, codes, w_router)
        d_gates = jnp.sum(select_own.astype(F32) * d_gate_back[:, :, None], axis=1)
        d_picked = (d_gates - jnp.sum(d_gates * gates, axis=0, keepdims=True)) / total * mask
        d_logits = (prob * (d_picked - jnp.sum(prob * d_picked, axis=0, keepdims=True))).astype(BF16)
        d_xn_two = (d_moe_in + mm('et,de->td', d_logits, w_router)).astype(BF16)
        grad_router = mm('td,et->de', xn_two, d_logits)
        d_hidden, grad_gain_ffn = norm_two_pull(d_xn_two)
        d_resid = (d_hidden + dy_own.astype(F32)).astype(BF16).reshape(num_seqs, seq_len, width)
        d_attn_out = mm('bse,de->bsd', d_resid, w_o).astype(BF16)
        d_qkv = attn_pull(d_attn_out)[0]
        foreign = lax.all_gather(jnp.stack(foreign), 'ep')
        d_xn_one = mm('bse,de->bsd', d_qkv, w_qkv).astype(BF16)
        d_x_norm, grad_gain_attn = norm_one_pull(d_xn_one)
        dx_out = (d_x_norm + d_resid.astype(F32)).astype(BF16)
        quarters = lambda arr: jnp.moveaxis(arr.reshape(tokens, 4, -1), 1, 0)
        dsend = jnp.concatenate([quarters(d_qkv), quarters(d_resid)], axis=2)
        gains = jnp.concatenate([grad_gain_attn, grad_gain_ffn]).reshape(-1, 128)
        world_size = planes * ep_size
        low, high, gains, grad_router = dense_sums(acts_xn, acts_ao, dsend, gains, grad_router.reshape(world_size, -1, 128))
        grad_router = grad_router.reshape(width, experts)
        grad_gain_attn, grad_gain_ffn = gains.reshape(2, width)

        flip = lambda arr, bit: lax.ppermute(arr, 'ep', [(e, e ^ bit) for e in range(ep_size)])
        low_x, high_y = flip(low, 2), flip(high, 4)
        low_y, high_x = flip(low, 4), flip(high, 2)
        low_xy, high_xy = flip(low_x, 4), flip(high_y, 2)
        pieces = [low, high, low_x, high_x, low_y, high_y, low_xy, high_xy]
        swapped = [flip(arr, 1) for arr in pieces[:6]]
        swapped += [flip(arr, 1) for arr in pieces[6:]]
        pieces = [arr for i in range(4) for arr in (pieces[2 * i], pieces[2 * i + 1], swapped[2 * i], swapped[2 * i + 1])]

        foreign = after(foreign, gains)
        recv, d_recv = dispatch_rows(foreign.reshape(-1, tokens, foreign.shape[-1]), router_t, recv, d_recv, ep_size * cap, cap)
        grads, first = (), 0
        for count in (local_exp // 4, local_exp // 4, local_exp // 2):
            grads = weight_grads(recv, d_recv, hid_own, w_up, w_lin, w_down, first, count, grads)
            first += count
        grad_up, grad_lin, grad_down = grads
        grad_wqkv, grad_wo = assemble(pieces)
        return (dx_out, grad_gain_attn, grad_wqkv, grad_wo, grad_gain_ffn, grad_router, grad_up, grad_lin, grad_down)

    in_specs = (tok_spec, tok_spec, tok_spec, rep_spec, rep_spec, rep_spec, rep_spec, rep_spec, exp_spec, exp_spec, exp_spec)
    out_specs = (tok_spec, rep_spec, rep_spec, rep_spec, rep_spec, rep_spec, exp_spec, exp_spec, exp_spec)

    return jax.shard_map(local, mesh=mesh, in_specs=in_specs, out_specs=out_specs, check_vma=False)
```
